128 devices in a mesh: head: 8 (over z_lo, x), blk: 16 (over z_hi, y, core).
Axes of the slice: x: 4, y: 4, z: 4 (z_hi: 2, z_lo: 2; z = z_hi * 2 + z_lo), core: 2. Of those that a mesh axis runs over, the one named last changes fastest.
Arguments:
- hidden_in: bfloat16 [8192, 4096], P(('blk', 'head')), may hold values from -6 to 6
- queries: bfloat16 [8192, 2048], P(('blk', 'head')), may hold values from -26 to 26
- key_states: bfloat16 [8192, 1024], P(('blk', 'head')), may hold values from -5 to 5
- value_states: bfloat16 [8192, 1024], P(('blk', 'head')), may hold values from -6 to 6
- out_weight: bfloat16 [2048, 4096], P('head'), may hold values from -0.125 to 0.125
- norm_gain: float32 [4096], replicated, may hold values from 0.1 to 1.9
- gate_weight: bfloat16 [4096, 7168], P(None, 'head'), may hold values from -0.09375 to 0.09375
- up_weight: bfloat16 [4096, 7168], P(None, 'head'), may hold values from -0.09375 to 0.09375
- down_weight: bfloat16 [7168, 4096], P('head'), may hold values from -0.0625 to 0.0625
Outputs:
- layer_out: bfloat16 [8192, 4096], P(('blk', 'head'))
The draws below stay inside these ranges and needn't reach their ends.
All inputs are finite; a program needn't handle non-finite values.
Results may differ from the reference program's by a relative error of at most 0.018.
Values may be sent and summed in bfloat16 or wider, within the bound.
No kernel may reach another device: no remote copies, remote signals or barrier semaphores. Data moves between devices by JAX's collectives and lax.ppermute only.
A program may use at most 192 MiB of HBM per device.

```python
import jax
import jax.numpy as jnp
from jax import lax

D = 4096
HEADS = 16
KV_HEADS = 8
HEAD_DIM = 128
FF = 7168
TOK_BLK = 512
SEQ = 8192


def paired_draw(seed_key):
    anchor = jax.random.fold_in(seed_key, 7)
    stream_keys = jax.random.fold_in(anchor, 1)
    stream_query = jax.random.fold_in(anchor, 2)
    key_width = KV_HEADS * HEAD_DIM
    query_width = HEADS * HEAD_DIM
    key_drawn = jnp.clip(jax.random.normal(stream_keys, (SEQ, key_width), jnp.float32), -5.0, 5.0)
    query_drawn = jnp.clip(2.5 * jax.random.normal(stream_query, (SEQ, query_width), jnp.float32), -15.0, 15.0)
    return (query_drawn, key_drawn)


def draw_queries(key, part):
    return paired_draw(key)[0].astype(jnp.bfloat16)


def draw_key_states(key, part):
    return paired_draw(key)[1].astype(jnp.bfloat16)


def levels(rng, extent, pieces, least, top_value):
    loudness = 1.0
    for axis_at, blocks in pieces:
        heights = jax.random.uniform(jax.random.fold_in(jax.random.fold_in(rng, 6), axis_at), (blocks,), jnp.float32, least / len(pieces), top_value / len(pieces))
        loudness = loudness * jnp.repeat(jnp.exp(heights), extent[axis_at] // blocks).reshape((-1,) + (1,) * (len(extent) - 1 - axis_at))
    return loudness


def normal_values(key, extent, width, reach, pieces=(), held_as=jnp.bfloat16):
    drawn = jax.random.normal(key, extent, jnp.float32) * width
    if len(pieces) > 0:
        drawn = levels(key, extent, pieces, -0.22, 0.18) * drawn
    return jnp.clip(drawn, min=-reach, max=reach).astype(held_as)


def setup_inputs(seed: int = 0) -> dict:
    splits = jax.random.split(jax.random.key(seed), 10)
    return {
        "hidden_in": normal_values(splits[0], (SEQ, D), 1.0, 6.0, ((0, 128),)),
        "queries": draw_queries(jax.random.fold_in(splits[9], 71), 0),
        "key_states": draw_key_states(jax.random.fold_in(splits[9], 71), 0),
        "value_states": normal_values(splits[3], (SEQ, KV_HEADS * HEAD_DIM), 1.0, 6.0, ((0, 128),)),
        "out_weight": normal_values(splits[4], (HEADS * HEAD_DIM, D), (HEADS * HEAD_DIM) ** -0.5, 0.125, ((0, 8),)),
        "norm_gain": jnp.clip(1.0 + 0.18 * jax.random.normal(splits[5], (D,), jnp.float32), 0.1, 1.9),
        "gate_weight": normal_values(splits[6], (D, FF), D ** -0.5, 0.09375, ((1, 8),)),
        "up_weight": normal_values(splits[7], (D, FF), D ** -0.5, 0.09375, ((1, 8),)),
        "down_weight": normal_values(splits[8], (FF, D), FF ** -0.5, 0.0625, ((0, 8),)),
    }


def attend_group(query_group, key_group, value_group):
    score_scale = HEAD_DIM ** (-0.5)
    positions = jnp.arange(SEQ, dtype=jnp.int32)

    def one_block(block_index):
        first_row = block_index * TOK_BLK
        query_block = lax.dynamic_slice_in_dim(query_group, first_row, TOK_BLK, 1)
        scores = jnp.einsum('rqd,kd->rqk', query_block, key_group) * score_scale
        query_pos = first_row + jnp.arange(TOK_BLK, dtype=jnp.int32)
        visible = positions[None, :] <= query_pos[:, None]
        row_peak = lax.optimization_barrier(jnp.max(jnp.where(visible, scores, -jnp.inf), axis=-1))
        exp_scores = jnp.where(visible, jnp.exp(scores - row_peak[..., None]), 0.0)
        row_total = lax.optimization_barrier(jnp.sum(exp_scores, axis=-1))
        rounded = lax.optimization_barrier(exp_scores.astype(jnp.bfloat16)).astype(jnp.float32)
        numerator = jnp.einsum('rqk,kd->rqd', rounded, value_group)
        return (numerator / row_total[..., None]).astype(jnp.bfloat16)
    return lax.map(one_block, jnp.arange(SEQ // TOK_BLK, dtype=jnp.int32))

def attend_tuple(groups):
    return attend_group(groups[0], groups[1], groups[2])

def reference(hidden_in, queries, key_states, value_states, out_weight, norm_gain, gate_weight, up_weight, down_weight):
    group_ratio = HEADS // KV_HEADS
    query_all = queries.astype(jnp.float32).reshape(SEQ, KV_HEADS, group_ratio, HEAD_DIM).transpose(1, 2, 0, 3)
    key_all = key_states.astype(jnp.float32).reshape(SEQ, KV_HEADS, HEAD_DIM).transpose(1, 0, 2)
    value_all = value_states.astype(jnp.float32).reshape(SEQ, KV_HEADS, HEAD_DIM).transpose(1, 0, 2)
    attended = lax.map(attend_tuple, (query_all, key_all, value_all))
    attended = attended.transpose(1, 3, 0, 2, 4).reshape(SEQ, HEADS * HEAD_DIM)
    projected = jnp.dot(attended, out_weight, preferred_element_type=jnp.float32)
    residual = (hidden_in.astype(jnp.float32) + projected).astype(jnp.bfloat16)
    widened = residual.astype(jnp.float32)
    mean_square = lax.optimization_barrier(jnp.mean(widened * widened, axis=-1, keepdims=True))
    normed = (widened * lax.rsqrt(mean_square + 1e-05) * norm_gain.astype(jnp.float32)).astype(jnp.bfloat16)
    gate_part = jnp.dot(normed, gate_weight, preferred_element_type=jnp.float32)
    up_part = jnp.dot(normed, up_weight, preferred_element_type=jnp.float32)
    inner_act = (jax.nn.silu(gate_part) * up_part).astype(jnp.bfloat16)
    mlp_out = jnp.dot(inner_act, down_weight, preferred_element_type=jnp.float32)
    return (residual.astype(jnp.float32) + mlp_out).astype(jnp.bfloat16)
```

```python
import jax
import jax.numpy as jnp
from jax import lax
from jax.experimental import pallas as pl
from jax.experimental.pallas import tpu as pltpu
from jax.sharding import PartitionSpec as P

HEAD_DIM = 128
BF = jnp.bfloat16
F32 = jnp.float32
NEG = -1e30
SCALE2 = HEAD_DIM**-0.5 * 1.4426950408889634
VLIM = 56 * 1024 * 1024


def flat(x, y, z, c):
    return ((z % 2) * 4 + x) * 16 + (z // 2) * 8 + y * 2 + c


def move(a, f):
    pairs = []
    for x in range(4):
        for y in range(4):
            for z in range(4):
                for c in range(2):
                    tx, ty, tz, tc = f(x, y, z, c)
                    pairs.append((flat(x, y, z, c), flat(tx % 4, ty % 4, tz % 4, tc)))
    return lax.ppermute(a, ("head", "blk"), pairs)


def x_by(d):
    return lambda x, y, z, c: (x + d, y, z, c)


def x_out(x, y, z, c):
    return (x + 1 if c == 0 else x - 1, y, z, c)


def core_swap(x, y, z, c):
    return (x, y, z, 1 - c)


def z_low_pair(x, y, z, c):
    return (x, y, z ^ 1, c)


def z_pair(x, y, z, c):
    return (x, y, z ^ 1 if c == 0 else 3 - z if z in (0, 3) else 3 - z, c)


def blk_by(dy, dz):
    return lambda x, y, z, c: (x, y + dy, z + 2 * dz, c)


def flash_body(q2, k, va, m_ref, acc_ref, qi, mask):
    for h in range(2):
        for r in range(2):
            rows = pl.ds(r * 256, 256)
            q = q2[qi, rows, h * 128 : (h + 1) * 128]
            s = lax.dot_general(q, k, (((1,), (1,)), ((), ())), preferred_element_type=F32)
            s = s * SCALE2
            if mask is not None:
                ri = lax.broadcasted_iota(jnp.int32, s.shape, 0) + r * 256
                ci = lax.broadcasted_iota(jnp.int32, s.shape, 1)
                s = jnp.where(ci <= ri, s, NEG)
            m_old = m_ref[qi, h, rows, :]
            m_new = jnp.maximum(m_old, jnp.max(s, axis=-1, keepdims=True))
            p = jnp.exp2(s - m_new[:, :1]).astype(BF)
            alpha = jnp.exp2(m_old - m_new)
            pv = jnp.dot(p, va, preferred_element_type=F32)
            acc = acc_ref[qi, h, rows, :]
            acc_ref[qi, h, rows, :] = acc * alpha[:, :1] + pv
            m_ref[qi, h, rows, :] = m_new


def flash_kernel(ids, q_own, q_oth, *refs):
    kvs, (o_own, ml_own, o_oth, ml_oth), (q2, kk, va, m_ref, acc_ref) = refs[:8], refs[8:12], refs[12:]
    q2[0] = q_own[...]
    q2[1] = q_oth[...]
    for j in range(8):
        kk[j] = kvs[j][:, :128]
        va[j, :, :128] = kvs[j][:, 128:]
        va[j, :, 128:] = jnp.ones((512, 128), BF)
    m_ref[...] = jnp.full(m_ref.shape, NEG, F32)
    acc_ref[...] = jnp.zeros(acc_ref.shape, F32)
    flash_body(q2, kk[0], va[0], m_ref, acc_ref, 0, True)

    def step(t, carry):
        qi = (t >= 7).astype(jnp.int32)
        j = jnp.where(t >= 7, t - 7, t + 1)

        @pl.when(ids[j] < ids[8 + qi])
        def _():
            flash_body(q2, kk[j], va[j], m_ref, acc_ref, qi, None)

        return carry

    lax.fori_loop(0, 15, step, 0)
    lane = lax.broadcasted_iota(jnp.int32, (512, 128), 1)
    for qi, o_ref, ml in ((0, o_own, ml_own), (1, o_oth, ml_oth)):
        lse = []
        for h in range(2):
            total = acc_ref[qi, h, :, 128:]
            seen = total > 0.0
            safe = jnp.where(seen, total, 1.0)
            o_ref[:, h * 128 : (h + 1) * 128] = (acc_ref[qi, h, :, :128] / safe).astype(o_ref.dtype)
            lse.append(jnp.where(seen, m_ref[qi, h] + jnp.log2(safe), NEG))
        ml[...] = jnp.where(lane == 0, lse[0], lse[1])


def flash(ids, q_own, q_oth, kvs):
    vm = pl.BlockSpec(memory_space=pltpu.VMEM)
    return pl.pallas_call(
        flash_kernel,
        in_specs=[pl.BlockSpec(memory_space=pltpu.SMEM)] + [vm] * 10,
        out_specs=[vm] * 4,
        out_shape=[
            jax.ShapeDtypeStruct((512, 256), F32),
            jax.ShapeDtypeStruct((512, 128), F32),
            jax.ShapeDtypeStruct((512, 256), BF),
            jax.ShapeDtypeStruct((512, 128), F32),
        ],
        scratch_shapes=[
            pltpu.VMEM((2, 512, 256), BF),
            pltpu.VMEM((8, 512, 128), BF),
            pltpu.VMEM((8, 512, 256), BF),
            pltpu.VMEM((2, 2, 512, 128), F32),
            pltpu.VMEM((2, 2, 512, 256), F32),
        ],
        compiler_params=pltpu.CompilerParams(vmem_limit_bytes=VLIM),
        cost_estimate=pl.CostEstimate(flops=8_600_000_000, transcendentals=0, bytes_accessed=4 << 20),
        name="flash",
    )(ids, q_own, q_oth, *kvs)


def merge_kernel(o_own, ml_own, o_in, ml_in, out):
    for h in range(2):
        a = ml_own[:, h : h + 1]
        b = ml_in[:, h : h + 1]
        top = jnp.maximum(a, b)
        wa = jnp.exp2(a - top)
        wb = jnp.exp2(b - top)
        tot = wa + wb
        cols = slice(h * 128, (h + 1) * 128)
        res = o_own[:, cols] * (wa / tot) + o_in[:, cols].astype(F32) * (wb / tot)
        res = res.astype(BF)
        for zl in range(2):
            for x in range(4):
                lo = (zl * 4 + x) * 64
                out[x, zl, :, cols] = res[lo : lo + 64]


def merge(*args):
    vm = pl.BlockSpec(memory_space=pltpu.VMEM)
    return pl.pallas_call(
        merge_kernel,
        in_specs=[vm] * 4,
        out_specs=vm,
        out_shape=jax.ShapeDtypeStruct((4, 2, 64, 256), BF),
        cost_estimate=pl.CostEstimate(flops=1_000_000, transcendentals=0, bytes_accessed=1 << 20),
        name="merge",
    )(*args)


def proj_kernel(ids, att, *refs):
    ws, (own, oth) = refs[:8], refs[8:]
    zl = ids[16]
    acc = jnp.zeros((128, own.shape[1]), F32)
    for k in range(8):
        xs = ids[k]
        cols = pl.ds(pl.multiple_of(ids[8 + k] * 128, 128), 128)
        a = jnp.concatenate([att[xs, zl, :, cols], att[xs, 1 - zl, :, cols]], axis=0)
        acc = acc + jnp.dot(a, ws[k][...], preferred_element_type=F32)
    own[...] = acc[:64]
    oth[...] = acc[64:].astype(BF)


def project(ids, att, own_w, ws):
    bn = 1024
    wspec = pl.BlockSpec((128, bn), lambda i: (0, i))
    return pl.pallas_call(
        proj_kernel,
        grid=(4096 // bn,),
        in_specs=[
            pl.BlockSpec(memory_space=pltpu.SMEM),
            pl.BlockSpec((4, 2, 64, 256), lambda i: (0, 0, 0, 0)),
            pl.BlockSpec((128, bn), lambda i: (0, i)),
            pl.BlockSpec((128, bn), lambda i: (1, i)),
        ]
        + [wspec] * 6,
        out_specs=[pl.BlockSpec((64, bn), lambda i: (0, i))] * 2,
        out_shape=[jax.ShapeDtypeStruct((64, 4096), F32), jax.ShapeDtypeStruct((64, 4096), BF)],
        compiler_params=pltpu.CompilerParams(vmem_limit_bytes=VLIM),
        cost_estimate=pl.CostEstimate(flops=1_100_000_000, transcendentals=0, bytes_accessed=9 << 20),
        name="project",
    )(ids, att, own_w, own_w, *ws)


def norm_kernel(hid, own, got, gain, res_out, nrm_out):
    res = (hid[...].astype(F32) + (own[...] + got[...].astype(F32))).astype(BF)
    res_out[...] = res
    wide = res.astype(F32)
    ms = jnp.mean(wide * wide, axis=-1, keepdims=True)
    nrm_out[...] = (wide * lax.rsqrt(ms + 1e-05) * gain[...]).astype(BF)


def residual_norm(hid, own, got, gain):
    vm = pl.BlockSpec(memory_space=pltpu.VMEM)
    return pl.pallas_call(
        norm_kernel,
        in_specs=[vm] * 4,
        out_specs=[vm] * 2,
        out_shape=[jax.ShapeDtypeStruct((64, 4096), BF)] * 2,
        cost_estimate=pl.CostEstimate(flops=2_000_000, transcendentals=0, bytes_accessed=3 << 20),
        name="norm",
    )(hid, own, got, gain)


def gate_up_kernel(*refs):
    xs, (wg, wu, out, ag, au) = refs[:4], refs[4:]
    i = pl.program_id(0)
    a = jnp.concatenate([r[...] for r in xs], axis=0)
    g = jnp.dot(a, wg[...], preferred_element_type=F32)
    u = jnp.dot(a, wu[...], preferred_element_type=F32)

    @pl.when(i == 0)
    def _():
        ag[...] = g
        au[...] = u

    @pl.when(i > 0)
    def _():
        ag[...] += g
        au[...] += u

    @pl.when(i == pl.num_programs(0) - 1)
    def _():
        gate = ag[...]
        out[...] = (gate / (1.0 + jnp.exp(-gate)) * au[...]).astype(BF)


def gate_up(xs, wg, wu):
    bk = 1024
    return pl.pallas_call(
        gate_up_kernel,
        grid=(4096 // bk,),
        in_specs=[pl.BlockSpec((64, bk), lambda i: (0, i))] * 4 + [pl.BlockSpec((bk, 896), lambda i: (i, 0))] * 2,
        out_specs=pl.BlockSpec((256, 896), lambda i: (0, 0)),
        out_shape=jax.ShapeDtypeStruct((256, 896), BF),
        scratch_shapes=[pltpu.VMEM((256, 896), F32)] * 2,
        compiler_params=pltpu.CompilerParams(vmem_limit_bytes=VLIM),
        cost_estimate=pl.CostEstimate(flops=3_760_000_000, transcendentals=0, bytes_accessed=16 << 20),
        name="gate_up",
    )(*xs, wg, wu)


def down_kernel(a1, w, *outs):
    res = jnp.dot(a1[...], w[...], preferred_element_type=F32).astype(BF)
    lo = 0
    for o in outs:
        n = o.shape[0]
        o[...] = res[lo : lo + n]
        lo += n


def down(inner, w, sizes):
    bn = 1024
    return pl.pallas_call(
        down_kernel,
        grid=(4096 // bn,),
        in_specs=[pl.BlockSpec((sum(sizes), 896), lambda i: (0, 0)), pl.BlockSpec((896, bn), lambda i: (0, i))],
        out_specs=[pl.BlockSpec((n, bn), lambda i: (0, i)) for n in sizes],
        out_shape=[jax.ShapeDtypeStruct((n, 4096), BF) for n in sizes],
        compiler_params=pltpu.CompilerParams(vmem_limit_bytes=VLIM),
        cost_estimate=pl.CostEstimate(flops=1_880_000_000, transcendentals=0, bytes_accessed=9 << 20),
        name="down",
    )(inner, w)


def added(a, b):
    return (a.astype(F32) + b.astype(F32)).astype(BF)


def exchange_qkv(queries, key_states, value_states):
    both = jnp.concatenate(
        [queries.reshape(64, 8, 256), key_states.reshape(64, 8, 128), value_states.reshape(64, 8, 128)], axis=2
    )
    got = lax.all_to_all(both, "head", split_axis=1, concat_axis=0, tiled=True)
    got = got.reshape(512, 512)
    return got[:, :256], got[:, 256:]


def local(hidden_in, queries, key_states, value_states, out_weight, norm_gain, gate_weight, up_weight, down_weight):
    head = lax.axis_index("head")
    blk = lax.axis_index("blk")
    x, zl = head % 4, head // 4
    c, y, zh = blk % 2, (blk // 2) % 4, blk // 8

    q_own, kv = exchange_qkv(queries, key_states, value_states)

    steps = [(1, 0), (-1, 0), (0, 1), (2, 0), (1, 1), (-1, 1), (2, 1)]
    kvs, key_ids = [kv], [blk]
    q_oth = move(q_own, core_swap)
    for dy, dz in steps:
        kvs.append(move(kv, blk_by(dy, dz)))
        key_ids.append((zh ^ dz) * 8 + ((y - dy) % 4) * 2 + c)
    ids = jnp.stack(key_ids + [blk, blk ^ 1]).astype(jnp.int32)

    w_own, kv_seen = lax.optimization_barrier((out_weight, kv))
    mine = lax.dynamic_slice_in_dim(w_own, c * 128, 128, 0)
    rest = lax.dynamic_slice_in_dim(w_own, (1 - c) * 128, 128, 0)
    g1a = move(mine, x_out)
    g1b = move(rest, x_out)
    g2 = move(g1a, x_out)
    s1a, s1b, s2 = move(g1a, core_swap), move(g1b, core_swap), move(g2, core_swap)
    side = jnp.where(c == 0, -1, 1)
    w_x = [x, x, x + side, x + side, x + 2, x - side, x - side, x + 2]
    w_half = [0, 1, c, 1 - c, c, 1 - c, c, 1 - c]
    w_ids = jnp.stack([jnp.asarray(v % 4, jnp.int32) for v in w_x] + [jnp.asarray(v, jnp.int32) for v in w_half] + [zl.astype(jnp.int32)])

    o_own, ml_own, o_oth, ml_oth = flash(ids, q_own, q_oth, kvs)
    o_in, ml_in = move(o_oth, core_swap), move(ml_oth, core_swap)
    att = merge(o_own, ml_own, o_in, ml_in)
    att = lax.all_to_all(att, "head", split_axis=0, concat_axis=0, axis_index_groups=[[0, 1, 2, 3], [4, 5, 6, 7]], tiled=True)
    own_sum, oth_sum = project(w_ids, att, out_weight, [g1a, g1b, g2, s1a, s1b, s2])
    got_sum = move(oth_sum, z_low_pair)
    residual, normed = residual_norm(hidden_in, own_sum, got_sum, norm_gain.reshape(1, 4096))

    n_p = move(normed, x_by(-1))
    n_m = move(normed, x_by(1))
    n_2 = move(normed, x_by(2))
    z_0 = move(normed, z_pair)
    z_p = move(n_p, z_pair)
    z_m = move(n_m, z_pair)
    z_2 = move(n_2, z_pair)
    inner_own = gate_up([n_2, n_p, n_m, normed], gate_weight, up_weight)
    inner_far = gate_up([z_2, z_p, z_m, z_0], gate_weight, up_weight)
    f_2, f_pm, f_0 = down(inner_far, down_weight, (64, 128, 64))
    p_2, p_pm, p_0 = down(inner_own, down_weight, (64, 128, 64))
    r_2 = move(added(p_2, move(f_2, z_pair)), x_by(2))
    q_pm = move(f_pm, z_pair)
    q_p = added(p_pm[:64], q_pm[:64])
    q_m = added(p_pm[64:], q_pm[64:])
    r_p = move(q_p, x_by(1))
    r_m = move(q_m, x_by(-1))
    q_0 = move(f_0, z_pair)
    total = p_0.astype(F32) + q_0.astype(F32) + r_2.astype(F32) + r_p.astype(F32) + r_m.astype(F32)
    return (residual.astype(F32) + total).astype(BF)


def solution(mesh):
    tok = P(("blk", "head"), None)
    return jax.shard_map(
        local,
        mesh=mesh,
        in_specs=(tok, tok, tok, tok, P("head", None), P(), P(None, "head"), P(None, "head"), P("head", None)),
        out_specs=tok,
        check_vma=False,
    )
```

```python
import functools

import jax
import jax.numpy as jnp
from jax import lax
from jax.experimental import pallas as pl
from jax.experimental.pallas import tpu as pltpu
from jax.sharding import PartitionSpec as P


HEAD_DIM = 128
BF = jnp.bfloat16
F32 = jnp.float32
NEG = -1e30
SCALE2 = HEAD_DIM**-0.5 * 1.4426950408889634
VLIM = 56 * 1024 * 1024


def flat(x, y, z, c):
    return ((z % 2) * 4 + x) * 16 + (z // 2) * 8 + y * 2 + c


def move(a, f):
    pairs = []
    for x in range(4):
        for y in range(4):
            for z in range(4):
                for c in range(2):
                    tx, ty, tz, tc = f(x, y, z, c)
                    pairs.append((flat(x, y, z, c), flat(tx % 4, ty % 4, tz % 4, tc)))
    return lax.ppermute(a, ("head", "blk"), pairs)


def x_by(d):
    return lambda x, y, z, c: (x + d, y, z, c)


def x_out(x, y, z, c):
    return (x + 1 if c == 0 else x - 1, y, z, c)


def core_swap(x, y, z, c):
    return (x, y, z, 1 - c)


def z_low_pair(x, y, z, c):
    return (x, y, z ^ 1, c)


def z_pair(x, y, z, c):
    return (x, y, z ^ 1 if c == 0 else 3 - z, c)


def blk_by(dy, dz):
    return lambda x, y, z, c: (x, y + dy, z + 2 * dz, c)


ROWS = 256


def flash_body(q2, k, va, m_ref, acc_ref, qi, mask):
    for h in range(2):
        for r in range(512 // ROWS):
            rows = pl.ds(r * ROWS, ROWS)
            q = q2[qi, rows, h * 128 : (h + 1) * 128]
            s = lax.dot_general(q, k, (((1,), (1,)), ((), ())), preferred_element_type=F32)
            if mask:
                ri = lax.broadcasted_iota(jnp.int32, s.shape, 0) + r * ROWS
                ci = lax.broadcasted_iota(jnp.int32, s.shape, 1)
                s = jnp.where(ci <= ri, s, NEG)
            m_old = m_ref[qi, h, rows, :]
            m_new = jnp.maximum(m_old, jnp.max(s, axis=-1, keepdims=True) * SCALE2)
            p = jnp.exp2(s * SCALE2 - m_new[:, :1]).astype(BF)
            alpha = jnp.exp2(m_old - m_new)
            pv = jnp.dot(p, va, preferred_element_type=F32)
            acc = acc_ref[qi, h, rows, :]
            acc_ref[qi, h, rows, :] = acc * jnp.concatenate([alpha, alpha], axis=1) + pv
            m_ref[qi, h, rows, :] = m_new


def flash_kernel(n, first, ids, q_own, q_oth, *refs):
    kvs, refs = refs[:n], refs[n:]
    if not first:
        init, refs = refs[:4], refs[4:]
    outs, (q2, kk, va, m_ref, acc_ref) = refs[:4], refs[4:]
    q2[0] = q_own[...]
    q2[1] = q_oth[...]
    for j in range(n):
        kk[j] = kvs[j][:, :128]
        va[j, :, :128] = kvs[j][:, 128:]
        va[j, :, 128:] = jnp.ones((512, 128), BF)
    if first:
        m_ref[...] = jnp.full(m_ref.shape, NEG, F32)
        acc_ref[...] = jnp.zeros(acc_ref.shape, F32)
        flash_body(q2, kk[0], va[0], m_ref, acc_ref, 0, True)
    else:
        for qi in range(2):
            for h in range(2):
                lse = jnp.broadcast_to(init[2 * qi + 1][:, h : h + 1], (512, 128))
                m_ref[qi, h] = lse
                acc_ref[qi, h, :, :128] = init[2 * qi][:, h * 128 : (h + 1) * 128]
                acc_ref[qi, h, :, 128:] = jnp.where(lse > NEG, 1.0, 0.0)

    lead = 1 if first else 0

    def step(t, carry):
        qi = (t >= n - lead).astype(jnp.int32)
        j = t - qi * (n - lead) + lead * (1 - qi)

        @pl.when(ids[j] < ids[n + qi])
        def _():
            flash_body(q2, kk[j], va[j], m_ref, acc_ref, qi, False)

        return carry

    lax.fori_loop(0, 2 * n - lead, step, 0)
    lane = lax.broadcasted_iota(jnp.int32, (512, 128), 1)
    for qi in range(2):
        o_ref, ml = outs[2 * qi], outs[2 * qi + 1]
        lse = []
        for h in range(2):
            total = acc_ref[qi, h, :, 128:]
            seen = total > 0.0
            safe = jnp.where(seen, total, 1.0)
            o_ref[:, h * 128 : (h + 1) * 128] = (acc_ref[qi, h, :, :128] / safe).astype(o_ref.dtype)
            lse.append(jnp.where(seen, m_ref[qi, h] + jnp.log2(safe), NEG))
        ml[...] = jnp.where(lane == 0, lse[0], lse[1])


def flash(ids, q_own, q_oth, kvs, init=None, last=True):
    vm = pl.BlockSpec(memory_space=pltpu.VMEM)
    n = len(kvs)
    extra = [] if init is None else list(init)
    oth = BF if last else F32
    return pl.pallas_call(
        functools.partial(flash_kernel, n, init is None),
        in_specs=[pl.BlockSpec(memory_space=pltpu.SMEM)] + [vm] * (2 + n + len(extra)),
        out_specs=[vm] * 4,
        out_shape=[
            jax.ShapeDtypeStruct((512, 256), F32),
            jax.ShapeDtypeStruct((512, 128), F32),
            jax.ShapeDtypeStruct((512, 256), oth),
            jax.ShapeDtypeStruct((512, 128), F32),
        ],
        scratch_shapes=[
            pltpu.VMEM((2, 512, 256), BF),
            pltpu.VMEM((n, 512, 128), BF),
            pltpu.VMEM((n, 512, 256), BF),
            pltpu.VMEM((2, 2, 512, 128), F32),
            pltpu.VMEM((2, 2, 512, 256), F32),
        ],
        compiler_params=pltpu.CompilerParams(vmem_limit_bytes=VLIM),
        cost_estimate=pl.CostEstimate(flops=1_100_000_000 * n, transcendentals=0, bytes_accessed=4 << 20),
    )(ids, q_own, q_oth, *kvs, *extra)


def merge_kernel(o_own, ml_own, o_in, ml_in, out):
    for h in range(2):
        a = ml_own[:, h : h + 1]
        b = ml_in[:, h : h + 1]
        top = jnp.maximum(a, b)
        wa = jnp.exp2(a - top)
        wb = jnp.exp2(b - top)
        tot = wa + wb
        cols = slice(h * 128, (h + 1) * 128)
        res = o_own[:, cols] * (wa / tot) + o_in[:, cols].astype(F32) * (wb / tot)
        res = res.astype(BF)
        for zl in range(2):
            for x in range(4):
                lo = (zl * 4 + x) * 64
                out[x, zl, :, cols] = res[lo : lo + 64]


def merge(*args):
    vm = pl.BlockSpec(memory_space=pltpu.VMEM)
    return pl.pallas_call(
        merge_kernel,
        in_specs=[vm] * 4,
        out_specs=vm,
        out_shape=jax.ShapeDtypeStruct((4, 2, 64, 256), BF),
        cost_estimate=pl.CostEstimate(flops=1_000_000, transcendentals=0, bytes_accessed=1 << 20),
        name="merge",
    )(*args)


def proj_kernel(ids, att, own_w, *refs):
    ws, (own, oth, wbuf, sems) = refs[:6], refs[6:]
    zl, c = ids[4], ids[5]
    near, far = pl.multiple_of(c * 128, 128), pl.multiple_of((1 - c) * 128, 128)
    lo, hi = pl.ds(near, 128), pl.ds(far, 128)
    copies = [(own_w.at[pl.ds(0, 128)], 0, pl.ds(0, 128)), (own_w.at[pl.ds(128, 128)], 0, pl.ds(128, 128))]
    copies += [(w, p, d) for w, p, d in zip(ws, (1, 1, 2, 2, 3, 3), (lo, hi, lo, hi, lo, hi))]
    dmas = [pltpu.make_async_copy(src, wbuf.at[p, d], sems.at[i]) for i, (src, p, d) in enumerate(copies)]
    for d in dmas[:PDEPTH]:
        d.start()
    for p in range(4):
        for i in (2 * p, 2 * p + 1):
            dmas[i].wait()
            if i + PDEPTH < 8:
                dmas[i + PDEPTH].start()
        xs = ids[p]
        a = jnp.concatenate([att[xs, zl], att[xs, 1 - zl]], axis=0)
        for n in range(4):
            cols = slice(n * 1024, (n + 1) * 1024)
            part = jnp.dot(a, wbuf[p, :, cols], preferred_element_type=F32)
            if p == 0:
                own[:, cols] = part[:64]
            else:
                own[:, cols] += part[:64]
            if p == 0:
                oth[:, cols] = part[64:]
            else:
                oth[:, cols] += part[64:]


def proj_outer(ids, att, own_w, *refs):
    ws, (own, oth, wbuf, acc, sems) = refs[:6], refs[6:]
    proj_kernel(ids, att, own_w, *ws, own, acc, wbuf, sems)
    oth[...] = acc[...].astype(BF)


def project(ids, att, own_w, ws):
    vm = pl.BlockSpec(memory_space=pltpu.VMEM)
    hb = pl.BlockSpec(memory_space=pltpu.HBM)
    return pl.pallas_call(
        proj_outer,
        in_specs=[pl.BlockSpec(memory_space=pltpu.SMEM), vm] + [hb] * 7,
        out_specs=[vm] * 2,
        out_shape=[jax.ShapeDtypeStruct((64, 4096), F32), jax.ShapeDtypeStruct((64, 4096), BF)],
        scratch_shapes=[
            pltpu.VMEM((4, 256, 4096), BF),
            pltpu.VMEM((64, 4096), F32),
            pltpu.SemaphoreType.DMA((8,)),
        ],
        compiler_params=pltpu.CompilerParams(vmem_limit_bytes=VLIM),
        cost_estimate=pl.CostEstimate(flops=1_100_000_000, transcendentals=0, bytes_accessed=9 << 20),
        name="project",
    )(ids, att, own_w, *ws)


def norm_kernel(hid, own, got, gain, res_out, nrm_out):
    res = (hid[...].astype(F32) + (own[...] + got[...].astype(F32))).astype(BF)
    res_out[...] = res
    wide = res.astype(F32)
    ms = jnp.mean(wide * wide, axis=-1, keepdims=True)
    nrm_out[...] = (wide * lax.rsqrt(ms + 1e-05) * gain[...]).astype(BF)


def residual_norm(hid, own, got, gain):
    vm = pl.BlockSpec(memory_space=pltpu.VMEM)
    return pl.pallas_call(
        norm_kernel,
        in_specs=[vm] * 4,
        out_specs=[vm] * 2,
        out_shape=[jax.ShapeDtypeStruct((64, 4096), BF)] * 2,
        cost_estimate=pl.CostEstimate(flops=2_000_000, transcendentals=0, bytes_accessed=3 << 20),
        name="norm",
    )(hid, own, got, gain)


KC = 1024
DEPTH = 4
PDEPTH = 8


def mlp_kernel(*refs):
    xs, (wg, wu, wd), outs, (wbuf, dbuf, acc, sems, dsems) = refs[:4], refs[4:7], refs[7:10], refs[10:]
    nk = 4096 // KC
    ups = []
    for k in range(nk):
        rows = pl.ds(k * KC, KC)
        ups.append(
            (
                pltpu.make_async_copy(wg.at[rows], wbuf.at[k, :, pl.ds(0, 896)], sems.at[k, 0]),
                pltpu.make_async_copy(wu.at[rows], wbuf.at[k, :, pl.ds(896, 896)], sems.at[k, 1]),
            )
        )
    downs = [pltpu.make_async_copy(wd.at[:, pl.ds(n * 1024, 1024)], dbuf.at[n], dsems.at[n]) for n in range(4)]
    order = [d for pair in ups for d in pair] + downs
    for d in order[:DEPTH]:
        d.start()

    def settle(at, count):
        for i in range(at, at + count):
            order[i].wait()
        for i in range(at + DEPTH, min(at + DEPTH + count, len(order))):
            order[i].start()

    for k in range(nk):
        settle(2 * k, 2)
        a = jnp.concatenate([r[:, k * KC : (k + 1) * KC] for r in xs], axis=0)
        part = jnp.dot(a, wbuf[k], preferred_element_type=F32)
        if k == 0:
            acc[...] = part
        else:
            acc[...] += part
    gate = acc[:, :896]
    inner = (gate / (1.0 + jnp.exp(-gate)) * acc[:, 896:]).astype(BF)
    for n in range(4):
        settle(2 * nk + n, 1)
        res = jnp.dot(inner, dbuf[n], preferred_element_type=F32).astype(BF)
        lo = 0
        for o in outs:
            m = o.shape[0]
            o[:, n * 1024 : (n + 1) * 1024] = res[lo : lo + m]
            lo += m


def mlp(xs, wg, wu, wd):
    vm = pl.BlockSpec(memory_space=pltpu.VMEM)
    hb = pl.BlockSpec(memory_space=pltpu.HBM)
    return pl.pallas_call(
        mlp_kernel,
        in_specs=[vm] * 4 + [hb] * 3,
        out_specs=[vm] * 3,
        out_shape=[jax.ShapeDtypeStruct((n, 4096), BF) for n in (64, 128, 64)],
        scratch_shapes=[
            pltpu.VMEM((4096 // KC, KC, 1792), BF),
            pltpu.VMEM((4, 896, 1024), BF),
            pltpu.VMEM((256, 1792), F32),
            pltpu.SemaphoreType.DMA((4096 // KC, 2)),
            pltpu.SemaphoreType.DMA((4,)),
        ],
        compiler_params=pltpu.CompilerParams(vmem_limit_bytes=VLIM),
        cost_estimate=pl.CostEstimate(flops=5_640_000_000, transcendentals=0, bytes_accessed=26 << 20),
    )(*xs, wg, wu, wd)


def added(a, b):
    return (a.astype(F32) + b.astype(F32)).astype(BF)


def exchange_qkv(queries, key_states, value_states):
    both = jnp.concatenate(
        [queries.reshape(64, 8, 256), key_states.reshape(64, 8, 128), value_states.reshape(64, 8, 128)], axis=2
    )
    got = lax.all_to_all(both, "head", split_axis=1, concat_axis=0, tiled=True)
    got = got.reshape(512, 512)
    return got[:, :256], got[:, 256:]


def local(hidden_in, queries, key_states, value_states, out_weight, norm_gain, gate_weight, up_weight, down_weight):
    head = lax.axis_index("head")
    blk = lax.axis_index("blk")
    x, zl = head % 4, head // 4
    c, y, zh = blk % 2, (blk // 2) % 4, blk // 8

    q_own, kv = exchange_qkv(queries, key_states, value_states)

    steps = [(1, 0), (-1, 0), (0, 1), (2, 0), (1, 1), (-1, 1), (2, 1)]
    kvs, key_ids = [kv], [blk]
    for i, (dy, dz) in enumerate(steps):
        kvs.append(move(kv, blk_by(dy, dz)))
        key_ids.append((zh ^ dz) * 8 + ((y - dy) % 4) * 2 + c)
        if i == 2:
            q_oth = move(q_own, core_swap)
    key_ids = [jnp.asarray(v, jnp.int32) for v in key_ids]
    ids_a = jnp.stack(key_ids[:4] + [blk, blk ^ 1])
    ids_b = jnp.stack(key_ids[4:] + [blk, blk ^ 1])

    mine = lax.dynamic_slice_in_dim(out_weight, c * 128, 128, 0)
    rest = lax.dynamic_slice_in_dim(out_weight, (1 - c) * 128, 128, 0)
    g1a = move(mine, x_out)
    g1b = move(rest, x_out)
    g2 = move(g1a, x_out)
    s1a, s1b, s2 = (move(g1a, core_swap), move(g1b, core_swap), move(g2, core_swap))
    side = jnp.where(c == 0, -1, 1)
    w_ids = jnp.stack([jnp.asarray(v, jnp.int32) for v in (x, (x + side) % 4, (x - side) % 4, (x + 2) % 4, zl, c)])

    state = flash(ids_a, q_own, q_oth, kvs[:4], None, False)
    o_own, ml_own, o_oth, ml_oth = flash(ids_b, q_own, q_oth, kvs[4:], state, True)
    o_in, ml_in = move(o_oth, core_swap), move(ml_oth, core_swap)
    att = merge(o_own, ml_own, o_in, ml_in)
    att = lax.all_to_all(att, "head", split_axis=0, concat_axis=0, axis_index_groups=[[0, 1, 2, 3], [4, 5, 6, 7]], tiled=True)
    own_sum, oth_sum = project(w_ids, att, out_weight, [g1a, g1b, s1b, s1a, g2, s2])
    got_sum = move(oth_sum, z_low_pair)
    residual, normed = residual_norm(hidden_in, own_sum, got_sum, norm_gain.reshape(1, 4096))

    n_p = move(normed, x_by(-1))
    n_m = move(normed, x_by(1))
    n_2 = move(normed, x_by(2))
    z_0 = move(normed, z_pair)
    z_p = move(n_p, z_pair)
    z_m = move(n_m, z_pair)
    z_2 = move(n_2, z_pair)
    weights = (gate_weight, up_weight, down_weight)
    p_2, p_pm, p_0 = mlp([n_2, n_p, n_m, normed], *weights)
    f_2, f_pm, f_0 = mlp([z_2, z_p, z_m, z_0], *weights)
    h_2 = move(f_2, z_pair)
    h_pm = move(f_pm, z_pair)
    h_0 = move(f_0, z_pair)
    r_2 = move(added(p_2, h_2), x_by(2))
    r_p = move(added(p_pm[:64], h_pm[:64]), x_by(1))
    r_m = move(added(p_pm[64:], h_pm[64:]), x_by(-1))
    total = p_0.astype(F32) + h_0.astype(F32) + r_2.astype(F32) + r_p.astype(F32) + r_m.astype(F32)
    return (residual.astype(F32) + total).astype(BF)


def solution(mesh):
    tok = P(("blk", "head"), None)
    return jax.shard_map(
        local,
        mesh=mesh,
        in_specs=(tok, tok, tok, tok, P("head", None), P(), P(None, "head"), P(None, "head"), P("head", None)),
        out_specs=tok,
        check_vma=False,
    )
```

```python
import functools

import jax
import jax.numpy as jnp
from jax import lax
from jax.experimental import pallas as pl
from jax.experimental.pallas import tpu as pltpu
from jax.sharding import PartitionSpec as P


HEAD_DIM = 128
BF = jnp.bfloat16
F32 = jnp.float32
NEG = -1e30
SCALE2 = HEAD_DIM**-0.5 * 1.4426950408889634
VLIM = 56 * 1024 * 1024


def flat(x, y, z, c):
    return ((z % 2) * 4 + x) * 16 + (z // 2) * 8 + y * 2 + c


def move(a, f):
    pairs = []
    for x in range(4):
        for y in range(4):
            for z in range(4):
                for c in range(2):
                    tx, ty, tz, tc = f(x, y, z, c)
                    pairs.append((flat(x, y, z, c), flat(tx % 4, ty % 4, tz % 4, tc)))
    return lax.ppermute(a, ("head", "blk"), pairs)


def x_by(d):
    return lambda x, y, z, c: (x + d, y, z, c)


def x_out(x, y, z, c):
    return (x + 1 if c == 0 else x - 1, y, z, c)


def x_in(x, y, z, c):
    return (x - 1 if c == 0 else x + 1, y, z, c)


def core_swap(x, y, z, c):
    return (x, y, z, 1 - c)


def z_low_pair(x, y, z, c):
    return (x, y, z ^ 1, c)


def z_pair(x, y, z, c):
    return (x, y, z ^ 1 if c == 0 else 3 - z, c)


def blk_by(dy, dz):
    return lambda x, y, z, c: (x, y + dy, z + 2 * dz, c)


ROWS = 128


GROUP = 2


def flash_body(q2, kk, va, m_ref, acc_ref, qi, slots, mask):
    for h in range(2):
        for r in range(512 // ROWS):
            rows = pl.ds(r * ROWS, ROWS)
            q = q2[qi, rows, h * 128 : (h + 1) * 128]
            ss = []
            for j in slots:
                s = lax.dot_general(q, kk[j], (((1,), (1,)), ((), ())), preferred_element_type=F32)
                if mask:
                    ri = lax.broadcasted_iota(jnp.int32, s.shape, 0) + r * ROWS
                    ci = lax.broadcasted_iota(jnp.int32, s.shape, 1)
                    s = jnp.where(ci <= ri, s, NEG)
                ss.append(s)
            top = ss[0]
            for s in ss[1:]:
                top = jnp.maximum(top, s)
            m_old = m_ref[qi, h, rows, :]
            m_new = jnp.maximum(m_old, jnp.max(top, axis=-1, keepdims=True) * SCALE2)
            pv = None
            for j, s in zip(slots, ss):
                p = jnp.exp2(s * SCALE2 - m_new[:, :1]).astype(BF)
                part = jnp.dot(p, va[j], preferred_element_type=F32)
                pv = part if pv is None else pv + part
            alpha = jnp.exp2(m_old - m_new)
            acc = acc_ref[qi, h, rows, :]
            acc_ref[qi, h, rows, :] = acc * jnp.concatenate([alpha, alpha], axis=1) + pv
            m_ref[qi, h, rows, :] = m_new


def flash_kernel(n, first, ids, q_own, q_oth, *refs):
    kvs, refs = refs[:n], refs[n:]
    if not first:
        init, refs = refs[:4], refs[4:]
    outs, (q2, kk, va, m_ref, acc_ref, vis) = refs[:4], refs[4:]
    q2[0] = q_own[...]
    q2[1] = q_oth[...]
    for j in range(n):
        kk[j] = kvs[j][:, :128]
        va[j, :, :128] = kvs[j][:, 128:]
        va[j, :, 128:] = jnp.ones((512, 128), BF)
    if first:
        m_ref[...] = jnp.full(m_ref.shape, NEG, F32)
        acc_ref[...] = jnp.zeros(acc_ref.shape, F32)
        flash_body(q2, kk, va, m_ref, acc_ref, 0, [0], True)
    else:
        for qi in range(2):
            for h in range(2):
                lse = jnp.broadcast_to(init[2 * qi + 1][:, h : h + 1], (512, 128))
                m_ref[qi, h] = lse
                acc_ref[qi, h, :, :128] = init[2 * qi][:, h * 128 : (h + 1) * 128]
                acc_ref[qi, h, :, 128:] = jnp.where(lse > NEG, 1.0, 0.0)

    counts = []
    for qi in range(2):
        seen = jnp.int32(0)
        for j in range(n):
            vis[qi, seen] = j
            seen = seen + (ids[j] < ids[n + qi]).astype(jnp.int32)
        counts.append(seen)
    groups = [cnt // GROUP for cnt in counts]

    def grouped(t, carry):
        qi = (t >= groups[0]).astype(jnp.int32)
        at = (t - qi * groups[0]) * GROUP
        flash_body(q2, kk, va, m_ref, acc_ref, qi, [vis[qi, at + g] for g in range(GROUP)], False)
        return carry

    lax.fori_loop(0, groups[0] + groups[1], grouped, 0)
    rest = [cnt - g * GROUP for cnt, g in zip(counts, groups)]

    def single(t, carry):
        qi = (t >= rest[0]).astype(jnp.int32)
        at = jnp.where(qi == 1, groups[1], groups[0]) * GROUP + t - qi * rest[0]
        flash_body(q2, kk, va, m_ref, acc_ref, qi, [vis[qi, at]], False)
        return carry

    lax.fori_loop(0, rest[0] + rest[1], single, 0)
    lane = lax.broadcasted_iota(jnp.int32, (512, 128), 1)
    for qi in range(2):
        o_ref, ml = outs[2 * qi], outs[2 * qi + 1]
        lse = []
        for h in range(2):
            total = acc_ref[qi, h, :, 128:]
            seen = total > 0.0
            safe = jnp.where(seen, total, 1.0)
            o_ref[:, h * 128 : (h + 1) * 128] = (acc_ref[qi, h, :, :128] / safe).astype(o_ref.dtype)
            lse.append(jnp.where(seen, m_ref[qi, h] + jnp.log2(safe), NEG))
        ml[...] = jnp.where(lane == 0, lse[0], lse[1])


def flash(ids, q_own, q_oth, kvs, init=None, last=True):
    vm = pl.BlockSpec(memory_space=pltpu.VMEM)
    n = len(kvs)
    extra = [] if init is None else list(init)
    oth = BF if last else F32
    return pl.pallas_call(
        functools.partial(flash_kernel, n, init is None),
        in_specs=[pl.BlockSpec(memory_space=pltpu.SMEM)] + [vm] * (2 + n + len(extra)),
        out_specs=[vm] * 4,
        out_shape=[
            jax.ShapeDtypeStruct((512, 256), F32),
            jax.ShapeDtypeStruct((512, 128), F32),
            jax.ShapeDtypeStruct((512, 256), oth),
            jax.ShapeDtypeStruct((512, 128), F32),
        ],
        scratch_shapes=[
            pltpu.VMEM((2, 512, 256), BF),
            pltpu.VMEM((n, 512, 128), BF),
            pltpu.VMEM((n, 512, 256), BF),
            pltpu.VMEM((2, 2, 512, 128), F32),
            pltpu.VMEM((2, 2, 512, 256), F32),
            pltpu.SMEM((2, n + 1), jnp.int32),
        ],
        compiler_params=pltpu.CompilerParams(vmem_limit_bytes=VLIM),
        cost_estimate=pl.CostEstimate(flops=1_100_000_000 * n, transcendentals=0, bytes_accessed=4 << 20),
    )(ids, q_own, q_oth, *kvs, *extra)


def merge_kernel(o_own, ml_own, o_in, ml_in, out):
    for h in range(2):
        a = ml_own[:, h : h + 1]
        b = ml_in[:, h : h + 1]
        top = jnp.maximum(a, b)
        wa = jnp.exp2(a - top)
        wb = jnp.exp2(b - top)
        tot = wa + wb
        cols = slice(h * 128, (h + 1) * 128)
        res = o_own[:, cols] * (wa / tot) + o_in[:, cols].astype(F32) * (wb / tot)
        res = res.astype(BF)
        for zl in range(2):
            for x in range(4):
                lo = (zl * 4 + x) * 64
                out[x, zl, :, cols] = res[lo : lo + 64]


def merge(*args):
    vm = pl.BlockSpec(memory_space=pltpu.VMEM)
    return pl.pallas_call(
        merge_kernel,
        in_specs=[vm] * 4,
        out_specs=vm,
        out_shape=jax.ShapeDtypeStruct((4, 2, 64, 256), BF),
        cost_estimate=pl.CostEstimate(flops=1_000_000, transcendentals=0, bytes_accessed=1 << 20),
        name="merge",
    )(*args)


def proj_kernel(ids, att, own_w, *refs):
    ws, (own, oth, wbuf, sems) = refs[:6], refs[6:]
    zl, c = ids[4], ids[5]
    near, far = pl.multiple_of(c * 128, 128), pl.multiple_of((1 - c) * 128, 128)
    lo, hi = pl.ds(near, 128), pl.ds(far, 128)
    copies = [(own_w.at[pl.ds(0, 128)], 0, pl.ds(0, 128)), (own_w.at[pl.ds(128, 128)], 0, pl.ds(128, 128))]
    copies += [(w, p, d) for w, p, d in zip(ws, (1, 1, 2, 2, 3, 3), (lo, hi, lo, hi, lo, hi))]
    dmas = [pltpu.make_async_copy(src, wbuf.at[p, d], sems.at[i]) for i, (src, p, d) in enumerate(copies)]
    for d in dmas[:PDEPTH]:
        d.start()
    for p in range(4):
        for i in (2 * p, 2 * p + 1):
            dmas[i].wait()
            if i + PDEPTH < 8:
                dmas[i + PDEPTH].start()
        xs = ids[p]
        a = jnp.concatenate([att[xs, zl], att[xs, 1 - zl]], axis=0)
        for n in range(4):
            cols = slice(n * 1024, (n + 1) * 1024)
            part = jnp.dot(a, wbuf[p, :, cols], preferred_element_type=F32)
            if p == 0:
                own[:, cols] = part[:64]
            else:
                own[:, cols] += part[:64]
            if p == 0:
                oth[:, cols] = part[64:]
            else:
                oth[:, cols] += part[64:]


def proj_outer(ids, att, own_w, *refs):
    ws, (own, oth, wbuf, acc, sems) = refs[:6], refs[6:]
    proj_kernel(ids, att, own_w, *ws, own, acc, wbuf, sems)
    oth[...] = acc[...].astype(BF)


def project(ids, att, own_w, ws):
    vm = pl.BlockSpec(memory_space=pltpu.VMEM)
    hb = pl.BlockSpec(memory_space=pltpu.HBM)
    return pl.pallas_call(
        proj_outer,
        in_specs=[pl.BlockSpec(memory_space=pltpu.SMEM), vm] + [hb] * 7,
        out_specs=[vm] * 2,
        out_shape=[jax.ShapeDtypeStruct((64, 4096), F32), jax.ShapeDtypeStruct((64, 4096), BF)],
        scratch_shapes=[
            pltpu.VMEM((4, 256, 4096), BF),
            pltpu.VMEM((64, 4096), F32),
            pltpu.SemaphoreType.DMA((8,)),
        ],
        compiler_params=pltpu.CompilerParams(vmem_limit_bytes=VLIM),
        cost_estimate=pl.CostEstimate(flops=1_100_000_000, transcendentals=0, bytes_accessed=9 << 20),
        name="project",
    )(ids, att, own_w, *ws)


def norm_kernel(hid, own, got, gain, res_out, nrm_out):
    res = (hid[...].astype(F32) + (own[...] + got[...].astype(F32))).astype(BF)
    res_out[...] = res
    wide = res.astype(F32)
    ms = jnp.mean(wide * wide, axis=-1, keepdims=True)
    nrm_out[...] = (wide * lax.rsqrt(ms + 1e-05) * gain[...]).astype(BF)


def residual_norm(hid, own, got, gain):
    vm = pl.BlockSpec(memory_space=pltpu.VMEM)
    return pl.pallas_call(
        norm_kernel,
        in_specs=[vm] * 4,
        out_specs=[vm] * 2,
        out_shape=[jax.ShapeDtypeStruct((64, 4096), BF)] * 2,
        cost_estimate=pl.CostEstimate(flops=2_000_000, transcendentals=0, bytes_accessed=3 << 20),
        name="norm",
    )(hid, own, got, gain)


KC = 1024
DEPTH = 4
PDEPTH = 8


def mlp_kernel(*refs):
    xs, (wg, wu, wd), outs, (wbuf, dbuf, acc, sems, dsems) = refs[:4], refs[4:7], refs[7:11], refs[11:]
    nk = 4096 // KC
    ups = []
    for k in range(nk):
        rows = pl.ds(k * KC, KC)
        ups.append(
            (
                pltpu.make_async_copy(wg.at[rows], wbuf.at[k, :, pl.ds(0, 896)], sems.at[k, 0]),
                pltpu.make_async_copy(wu.at[rows], wbuf.at[k, :, pl.ds(896, 896)], sems.at[k, 1]),
            )
        )
    downs = [pltpu.make_async_copy(wd.at[:, pl.ds(n * 1024, 1024)], dbuf.at[n], dsems.at[n]) for n in range(4)]
    order = [d for pair in ups for d in pair] + downs
    for d in order[:DEPTH]:
        d.start()

    def settle(at, count):
        for i in range(at, at + count):
            order[i].wait()
        for i in range(at + DEPTH, min(at + DEPTH + count, len(order))):
            order[i].start()

    for k in range(nk):
        settle(2 * k, 2)
        a = jnp.concatenate([r[:, k * KC : (k + 1) * KC] for r in xs], axis=0)
        part = jnp.dot(a, wbuf[k], preferred_element_type=F32)
        if k == 0:
            acc[...] = part
        else:
            acc[...] += part
    gate = acc[:, :896]
    inner = (gate / (1.0 + jnp.exp(-gate)) * acc[:, 896:]).astype(BF)
    for n in range(4):
        settle(2 * nk + n, 1)
        res = jnp.dot(inner, dbuf[n], preferred_element_type=F32).astype(BF)
        lo = 0
        for o in outs:
            m = o.shape[0]
            o[:, n * 1024 : (n + 1) * 1024] = res[lo : lo + m]
            lo += m


def mlp(xs, wg, wu, wd):
    vm = pl.BlockSpec(memory_space=pltpu.VMEM)
    hb = pl.BlockSpec(memory_space=pltpu.HBM)
    return pl.pallas_call(
        mlp_kernel,
        in_specs=[vm] * 4 + [hb] * 3,
        out_specs=[vm] * 4,
        out_shape=[jax.ShapeDtypeStruct((64, 4096), BF)] * 4,
        scratch_shapes=[
            pltpu.VMEM((4096 // KC, KC, 1792), BF),
            pltpu.VMEM((4, 896, 1024), BF),
            pltpu.VMEM((256, 1792), F32),
            pltpu.SemaphoreType.DMA((4096 // KC, 2)),
            pltpu.SemaphoreType.DMA((4,)),
        ],
        compiler_params=pltpu.CompilerParams(vmem_limit_bytes=VLIM),
        cost_estimate=pl.CostEstimate(flops=5_640_000_000, transcendentals=0, bytes_accessed=26 << 20),
    )(*xs, wg, wu, wd)


def added(a, b):
    return (a.astype(F32) + b.astype(F32)).astype(BF)


def pack_kernel(q, k, v, out):
    for h in range(8):
        out[h, :, :256] = q[:, h * 256 : (h + 1) * 256]
        out[h, :, 256:384] = k[:, h * 128 : (h + 1) * 128]
        out[h, :, 384:] = v[:, h * 128 : (h + 1) * 128]


def exchange_qkv(queries, key_states, value_states):
    vm = pl.BlockSpec(memory_space=pltpu.VMEM)
    both = pl.pallas_call(
        pack_kernel,
        in_specs=[vm] * 3,
        out_specs=vm,
        out_shape=jax.ShapeDtypeStruct((8, 64, 512), BF),
        cost_estimate=pl.CostEstimate(flops=1_000_000, transcendentals=0, bytes_accessed=1 << 20),
        name="pack",
    )(queries, key_states, value_states)
    got = lax.all_to_all(both, "head", split_axis=0, concat_axis=0, tiled=True)
    got = got.reshape(512, 512)
    return got[:, :256], got[:, 256:]


def local(hidden_in, queries, key_states, value_states, out_weight, norm_gain, gate_weight, up_weight, down_weight):
    head = lax.axis_index("head")
    blk = lax.axis_index("blk")
    x, zl = head % 4, head // 4
    c, y, zh = blk % 2, (blk // 2) % 4, blk // 8

    q_own, kv = exchange_qkv(queries, key_states, value_states)

    steps = [(1, 0), (-1, 0), (0, 1), (2, 0), (1, 1), (-1, 1), (2, 1)]
    kvs, key_ids = [kv], [blk]
    for i, (dy, dz) in enumerate(steps):
        kvs.append(move(kv, blk_by(dy, dz)))
        key_ids.append((zh ^ dz) * 8 + ((y - dy) % 4) * 2 + c)
        if i == 2:
            q_oth = move(q_own, core_swap)
    key_ids = [jnp.asarray(v, jnp.int32) for v in key_ids]
    ids_a = jnp.stack(key_ids[:4] + [blk, blk ^ 1])
    ids_b = jnp.stack(key_ids[4:] + [blk, blk ^ 1])

    mine = lax.dynamic_slice_in_dim(out_weight, c * 128, 128, 0)
    rest = lax.dynamic_slice_in_dim(out_weight, (1 - c) * 128, 128, 0)
    g1a = move(mine, x_out)
    g1b = move(rest, x_out)
    g2 = move(g1a, x_out)
    s1a, s1b, s2 = (move(g1a, core_swap), move(g1b, core_swap), move(g2, core_swap))
    side = jnp.where(c == 0, -1, 1)
    w_ids = jnp.stack([jnp.asarray(v, jnp.int32) for v in (x, (x + side) % 4, (x - side) % 4, (x + 2) % 4, zl, c)])

    state = flash(ids_a, q_own, q_oth, kvs[:4], None, False)
    o_own, ml_own, o_oth, ml_oth = flash(ids_b, q_own, q_oth, kvs[4:], state, True)
    o_in, ml_in = move(o_oth, core_swap), move(ml_oth, core_swap)
    att = merge(o_own, ml_own, o_in, ml_in)
    att = lax.all_to_all(
        att, "head", split_axis=0, concat_axis=0, axis_index_groups=[[0, 1, 2, 3], [4, 5, 6, 7]], tiled=True
    )
    own_sum, oth_sum = project(w_ids, att, out_weight, [g1a, g1b, s1b, s1a, g2, s2])
    got_sum = move(oth_sum, z_low_pair)
    residual, normed = residual_norm(hidden_in, own_sum, got_sum, norm_gain.reshape(1, 4096))

    n_a = move(normed, x_out)
    n_b = move(normed, x_in)
    z_0 = move(normed, z_pair)
    n_2 = move(n_a, x_out)
    z_a = move(n_a, z_pair)
    z_b = move(n_b, z_pair)
    z_2 = move(n_2, z_pair)
    weights = (gate_weight, up_weight, down_weight)
    p_0, p_a, p_b, f_0 = mlp([normed, n_a, n_b, z_0], *weights)
    h_0 = move(f_0, z_pair)
    f_2, f_a, f_b, p_2 = mlp([z_2, z_a, z_b, n_2], *weights)
    h_2 = move(f_2, z_pair)
    h_a = move(f_a, z_pair)
    h_b = move(f_b, z_pair)
    r_2 = move(added(p_2, h_2), x_by(2))
    r_a = move(added(p_a, h_a), x_in)
    r_b = move(added(p_b, h_b), x_out)
    total = p_0.astype(F32) + h_0.astype(F32) + r_2.astype(F32) + r_a.astype(F32) + r_b.astype(F32)
    return (residual.astype(F32) + total).astype(BF)


def solution(mesh):
    tok = P(("blk", "head"), None)
    return jax.shard_map(
        local,
        mesh=mesh,
        in_specs=(tok, tok, tok, tok, P("head", None), P(), P(None, "head"), P(None, "head"), P("head", None)),
        out_specs=tok,
        check_vma=False,
    )
```

```python
import functools

import jax
import jax.numpy as jnp
from jax import lax
from jax.experimental import pallas as pl
from jax.experimental.pallas import tpu as pltpu
from jax.sharding import PartitionSpec as P


HEAD_DIM = 128
BF = jnp.bfloat16
F32 = jnp.float32
NEG = -1e30
SCALE2 = HEAD_DIM**-0.5 * 1.4426950408889634
VLIM = 56 * 1024 * 1024
MLP_VLIM = 66_000_000


def flat(x, y, z, c):
    return ((z % 2) * 4 + x) * 16 + (z // 2) * 8 + y * 2 + c


def move(a, f):
    pairs = []
    for x in range(4):
        for y in range(4):
            for z in range(4):
                for c in range(2):
                    tx, ty, tz, tc = f(x, y, z, c)
                    pairs.append((flat(x, y, z, c), flat(tx % 4, ty % 4, tz % 4, tc)))
    return lax.ppermute(a, ("head", "blk"), pairs)


def x_by(d):
    return lambda x, y, z, c: (x + d, y, z, c)


def x_out(x, y, z, c):
    return (x + 1 if c == 0 else x - 1, y, z, c)


def x_in(x, y, z, c):
    return (x - 1 if c == 0 else x + 1, y, z, c)


def core_swap(x, y, z, c):
    return (x, y, z, 1 - c)


def z_low_pair(x, y, z, c):
    return (x, y, z ^ 1, c)


def z_pair(x, y, z, c):
    return (x, y, z ^ 1 if c == 0 else 3 - z, c)


def blk_by(dy, dz):
    return lambda x, y, z, c: (x, y + dy, z + 2 * dz, c)


ROWS = 128


GROUP = 2


def flash_body(q2, kk, va, m_ref, acc_ref, qi, slots, mask):
    for h in range(2):
        for r in range(512 // ROWS):
            rows = pl.ds(r * ROWS, ROWS)
            q = q2[qi, rows, h * 128 : (h + 1) * 128]
            ss = []
            for j in slots:
                s = lax.dot_general(q, kk[j], (((1,), (1,)), ((), ())), preferred_element_type=F32)
                if mask:
                    ri = lax.broadcasted_iota(jnp.int32, s.shape, 0) + r * ROWS
                    ci = lax.broadcasted_iota(jnp.int32, s.shape, 1)
                    s = jnp.where(ci <= ri, s, NEG)
                ss.append(s)
            top = ss[0]
            for s in ss[1:]:
                top = jnp.maximum(top, s)
            m_old = m_ref[qi, h, rows, :]
            m_new = jnp.maximum(m_old, jnp.max(top, axis=-1, keepdims=True) * SCALE2)
            pv = None
            for j, s in zip(slots, ss):
                p = jnp.exp2(s * SCALE2 - m_new[:, :1]).astype(BF)
                part = jnp.dot(p, va[j], preferred_element_type=F32)
                pv = part if pv is None else pv + part
            alpha = jnp.exp2(m_old - m_new)
            acc = acc_ref[qi, h, rows, :]
            acc_ref[qi, h, rows, :] = acc * jnp.concatenate([alpha, alpha], axis=1) + pv
            m_ref[qi, h, rows, :] = m_new


def flash_kernel(n, first, base, table, q_own, q_oth, *refs):
    ids = [table[base + j] for j in range(n)] + [table[8], table[9]]
    kvs, refs = refs[:n], refs[n:]
    if not first:
        init, refs = refs[:4], refs[4:]
    outs, (q2, kk, va, m_ref, acc_ref, vis) = refs[:4], refs[4:]
    q2[0] = q_own[...]
    q2[1] = q_oth[...]
    for j in range(n):
        kk[j] = kvs[j][:, :128]
        va[j, :, :128] = kvs[j][:, 128:]
        va[j, :, 128:] = jnp.ones((512, 128), BF)
    if first:
        m_ref[...] = jnp.full(m_ref.shape, NEG, F32)
        acc_ref[...] = jnp.zeros(acc_ref.shape, F32)
        flash_body(q2, kk, va, m_ref, acc_ref, 0, [0], True)
    else:
        for qi in range(2):
            for h in range(2):
                lse = jnp.broadcast_to(init[2 * qi + 1][:, h : h + 1], (512, 128))
                m_ref[qi, h] = lse
                acc_ref[qi, h, :, :128] = init[2 * qi][:, h * 128 : (h + 1) * 128]
                acc_ref[qi, h, :, 128:] = jnp.where(lse > NEG, 1.0, 0.0)

    counts = []
    for qi in range(2):
        seen = jnp.int32(0)
        for j in range(n):
            vis[qi, seen] = j
            seen = seen + (ids[j] < ids[n + qi]).astype(jnp.int32)
        counts.append(seen)
    groups = [cnt // GROUP for cnt in counts]

    def grouped(t, carry):
        qi = (t >= groups[0]).astype(jnp.int32)
        at = (t - qi * groups[0]) * GROUP
        flash_body(q2, kk, va, m_ref, acc_ref, qi, [vis[qi, at + g] for g in range(GROUP)], False)
        return carry

    lax.fori_loop(0, groups[0] + groups[1], grouped, 0)
    rest = [cnt - g * GROUP for cnt, g in zip(counts, groups)]

    def single(t, carry):
        qi = (t >= rest[0]).astype(jnp.int32)
        at = jnp.where(qi == 1, groups[1], groups[0]) * GROUP + t - qi * rest[0]
        flash_body(q2, kk, va, m_ref, acc_ref, qi, [vis[qi, at]], False)
        return carry

    lax.fori_loop(0, rest[0] + rest[1], single, 0)
    lane = lax.broadcasted_iota(jnp.int32, (512, 128), 1)
    for qi in range(2):
        o_ref, ml = outs[2 * qi], outs[2 * qi + 1]
        lse = []
        for h in range(2):
            total = acc_ref[qi, h, :, 128:]
            seen = total > 0.0
            safe = jnp.where(seen, total, 1.0)
            o_ref[:, h * 128 : (h + 1) * 128] = (acc_ref[qi, h, :, :128] / safe).astype(o_ref.dtype)
            lse.append(jnp.where(seen, m_ref[qi, h] + jnp.log2(safe), NEG))
        ml[...] = jnp.where(lane == 0, lse[0], lse[1])


def flash(ids, base, q_own, q_oth, kvs, init=None, last=True):
    vm = pl.BlockSpec(memory_space=pltpu.VMEM)
    n = len(kvs)
    extra = [] if init is None else list(init)
    oth = BF if last else F32
    return pl.pallas_call(
        functools.partial(flash_kernel, n, init is None, base),
        in_specs=[pl.BlockSpec(memory_space=pltpu.SMEM)] + [vm] * (2 + n + len(extra)),
        out_specs=[vm] * 4,
        out_shape=[
            jax.ShapeDtypeStruct((512, 256), F32),
            jax.ShapeDtypeStruct((512, 128), F32),
            jax.ShapeDtypeStruct((512, 256), oth),
            jax.ShapeDtypeStruct((512, 128), F32),
        ],
        scratch_shapes=[
            pltpu.VMEM((2, 512, 256), BF),
            pltpu.VMEM((n, 512, 128), BF),
            pltpu.VMEM((n, 512, 256), BF),
            pltpu.VMEM((2, 2, 512, 128), F32),
            pltpu.VMEM((2, 2, 512, 256), F32),
            pltpu.SMEM((2, n + 1), jnp.int32),
        ],
        compiler_params=pltpu.CompilerParams(vmem_limit_bytes=VLIM),
        cost_estimate=pl.CostEstimate(flops=1_100_000_000 * n, transcendentals=0, bytes_accessed=4 << 20),
    )(ids, q_own, q_oth, *kvs, *extra)


def merge_kernel(ids, o_own, ml_own, o_in, ml_in, *outs):
    for d, out in enumerate(outs):
        for zl in range(2):
            rows = pl.ds(pl.multiple_of(zl * 256 + ids[10 + d] * 64, 64), 64)
            for h in range(2):
                a = ml_own[rows, h : h + 1]
                b = ml_in[rows, h : h + 1]
                top = jnp.maximum(a, b)
                wa = jnp.exp2(a - top)
                wb = jnp.exp2(b - top)
                tot = wa + wb
                cols = slice(h * 128, (h + 1) * 128)
                res = o_own[rows, cols] * (wa / tot) + o_in[rows, cols].astype(F32) * (wb / tot)
                out[zl, :, cols] = res.astype(BF)


def merge(*args):
    vm = pl.BlockSpec(memory_space=pltpu.VMEM)
    return pl.pallas_call(
        merge_kernel,
        in_specs=[pl.BlockSpec(memory_space=pltpu.SMEM)] + [vm] * 4,
        out_specs=[vm] * 4,
        out_shape=[jax.ShapeDtypeStruct((2, 64, 256), BF)] * 4,
        cost_estimate=pl.CostEstimate(flops=1_000_000, transcendentals=0, bytes_accessed=1 << 20),
        name="merge",
    )(*args)


def proj_kernel(col, ids, att0, att1, att2, att3, own_w, *refs):
    atts, ws, (own, oth, wbuf, acc, sems) = (att0, att1, att2, att3), refs[:6], refs[6:]
    zl, c = ids[14], ids[15]
    width = own.shape[1]
    near, far = pl.multiple_of(c * 128, 128), pl.multiple_of((1 - c) * 128, 128)
    lo, hi = pl.ds(near, 128), pl.ds(far, 128)
    cut = pl.ds(col, width)
    copies = [(own_w.at[pl.ds(0, 256), cut], 0, pl.ds(0, 256))]
    copies += [(w.at[:, cut], p, d) for w, p, d in zip(ws, (1, 1, 2, 2, 3, 3), (lo, hi, lo, hi, lo, hi))]
    dmas = [pltpu.make_async_copy(src, wbuf.at[p, d], sems.at[i]) for i, (src, p, d) in enumerate(copies)]
    for d in dmas:
        d.start()
    for p in range(4):
        for i in (0,) if p == 0 else (2 * p - 1, 2 * p):
            dmas[i].wait()
        att = atts[p]
        a = jnp.concatenate([att[zl], att[1 - zl]], axis=0)
        part = jnp.dot(a, wbuf[p], preferred_element_type=F32)
        if p == 0:
            acc[...] = part
        else:
            acc[...] += part
    own[...] = acc[:64]
    oth[...] = acc[64:].astype(BF)


def project(ids, atts, own_w, ws, col, width):
    vm = pl.BlockSpec(memory_space=pltpu.VMEM)
    hb = pl.BlockSpec(memory_space=pltpu.HBM)
    return pl.pallas_call(
        functools.partial(proj_kernel, col),
        in_specs=[pl.BlockSpec(memory_space=pltpu.SMEM)] + [vm] * 4 + [hb] * 7,
        out_specs=[vm] * 2,
        out_shape=[jax.ShapeDtypeStruct((64, width), F32), jax.ShapeDtypeStruct((64, width), BF)],
        scratch_shapes=[
            pltpu.VMEM((4, 256, width), BF),
            pltpu.VMEM((128, width), F32),
            pltpu.SemaphoreType.DMA((7,)),
        ],
        compiler_params=pltpu.CompilerParams(vmem_limit_bytes=VLIM),
        cost_estimate=pl.CostEstimate(flops=550_000_000, transcendentals=0, bytes_accessed=4 << 20),
    )(ids, *atts, own_w, *ws)


def norm_kernel(hid, own, got, gain, res_out, nrm_out):
    res = (hid[...].astype(F32) + (own[...] + got[...].astype(F32))).astype(BF)
    res_out[...] = res
    wide = res.astype(F32)
    ms = jnp.mean(wide * wide, axis=-1, keepdims=True)
    nrm_out[...] = (wide * lax.rsqrt(ms + 1e-05) * gain[...]).astype(BF)


def residual_norm(*args):
    vm = pl.BlockSpec(memory_space=pltpu.VMEM)
    return pl.pallas_call(
        norm_kernel,
        in_specs=[vm] * 4,
        out_specs=[vm] * 2,
        out_shape=[jax.ShapeDtypeStruct((64, 4096), BF)] * 2,
        cost_estimate=pl.CostEstimate(flops=2_000_000, transcendentals=0, bytes_accessed=3 << 20),
        name="norm",
    )(*args)


KC = 1024
DEPTH = 4


def mlp_kernel(n_in, *refs):
    xs, (wg, wu, wd), outs = refs[:n_in], refs[n_in : n_in + 3], refs[n_in + 3 : 3 * n_in + 3]
    wbuf, dbuf, acc, xbuf, obuf, sems, xsems, osems = refs[3 * n_in + 3 :]
    nk = 4096 // KC
    order = []
    for k in range(nk):
        rows = pl.ds(k * KC, KC)
        order.append(pltpu.make_async_copy(wg.at[rows], wbuf.at[k, :, pl.ds(0, 896)], sems.at[2 * k]))
        order.append(pltpu.make_async_copy(wu.at[rows], wbuf.at[k, :, pl.ds(896, 896)], sems.at[2 * k + 1]))
    order += [
        pltpu.make_async_copy(wd.at[:, pl.ds(n * 1024, 1024)], dbuf.at[n], sems.at[2 * nk + n]) for n in range(4)
    ]
    loads = [pltpu.make_async_copy(r, xbuf.at[pl.ds(i * 64, 64)], xsems.at[i]) for i, r in enumerate(xs)]
    for d in loads + order[:DEPTH]:
        d.start()

    def settle(at, count):
        for i in range(at, at + count):
            order[i].wait()
        for i in range(at + DEPTH, min(at + DEPTH + count, len(order))):
            order[i].start()

    for d in loads:
        d.wait()
    for k in range(nk):
        settle(2 * k, 2)
        part = jnp.dot(xbuf[:, k * KC : (k + 1) * KC], wbuf[k], preferred_element_type=F32)
        if k == 0:
            acc[...] = part
        else:
            acc[...] += part
    gate = acc[:, :896]
    inner = (gate / (1.0 + jnp.exp(-gate)) * acc[:, 896:]).astype(BF)
    stores = []
    for n in range(4):
        settle(2 * nk + n, 1)
        cols = pl.ds(n * 1024, 1024)
        obuf[:, n * 1024 : (n + 1) * 1024] = jnp.dot(inner, dbuf[n], preferred_element_type=F32).astype(BF)
        at = pl.ds(n % 2 * 1024, 1024)
        for i in range(n_in):
            o = outs[2 * i + n // 2]
            d = pltpu.make_async_copy(obuf.at[pl.ds(i * 64, 64), cols], o.at[:, at], osems.at[n, i])
            d.start()
            stores.append(d)
    for d in stores:
        d.wait()


def mlp(xs, wg, wu, wd):
    hb = pl.BlockSpec(memory_space=pltpu.HBM)
    n_in = len(xs)
    return pl.pallas_call(
        functools.partial(mlp_kernel, n_in),
        in_specs=[hb] * (n_in + 3),
        out_specs=[hb] * (2 * n_in),
        out_shape=[jax.ShapeDtypeStruct((64, 2048), BF)] * (2 * n_in),
        scratch_shapes=[
            pltpu.VMEM((4096 // KC, KC, 1792), BF),
            pltpu.VMEM((4, 896, 1024), BF),
            pltpu.VMEM((n_in * 64, 1792), F32),
            pltpu.VMEM((n_in * 64, 4096), BF),
            pltpu.VMEM((n_in * 64, 4096), BF),
            pltpu.SemaphoreType.DMA((2 * (4096 // KC) + 4,)),
            pltpu.SemaphoreType.DMA((n_in,)),
            pltpu.SemaphoreType.DMA((4, n_in)),
        ],
        compiler_params=pltpu.CompilerParams(vmem_limit_bytes=MLP_VLIM),
        cost_estimate=pl.CostEstimate(flops=5_640_000_000, transcendentals=0, bytes_accessed=26 << 20),
    )(*xs, wg, wu, wd)


def added(a, b):
    return (a.astype(F32) + b.astype(F32)).astype(BF)


def pack_kernel(q, k, v, out):
    for h in range(8):
        out[h, :, :256] = q[:, h * 256 : (h + 1) * 256]
        out[h, :, 256:384] = k[:, h * 128 : (h + 1) * 128]
        out[h, :, 384:] = v[:, h * 128 : (h + 1) * 128]


def exchange_qkv(queries, key_states, value_states):
    vm = pl.BlockSpec(memory_space=pltpu.VMEM)
    both = pl.pallas_call(
        pack_kernel,
        in_specs=[vm] * 3,
        out_specs=vm,
        out_shape=jax.ShapeDtypeStruct((8, 64, 512), BF),
        cost_estimate=pl.CostEstimate(flops=1_000_000, transcendentals=0, bytes_accessed=1 << 20),
        name="pack",
    )(queries, key_states, value_states)
    got = lax.all_to_all(both, "head", split_axis=0, concat_axis=0, tiled=True)
    got = got.reshape(512, 512)
    return got[:, :256], got[:, 256:]


def local(hidden_in, queries, key_states, value_states, out_weight, norm_gain, gate_weight, up_weight, down_weight):
    head = lax.axis_index("head")
    blk = lax.axis_index("blk")
    x, zl = head % 4, head // 4
    c, y, zh = blk % 2, (blk // 2) % 4, blk // 8

    q_own, kv = exchange_qkv(queries, key_states, value_states)

    steps = [(1, 0), (-1, 0), (0, 1), (2, 0), (1, 1), (-1, 1), (2, 1)]
    kvs, key_ids = [kv], [blk]
    for dy, dz in steps:
        kvs.append(move(kv, blk_by(dy, dz)))
        key_ids.append((zh ^ dz) * 8 + ((y - dy) % 4) * 2 + c)
    q_oth = move(q_own, core_swap)
    side = jnp.where(c == 0, 1, -1)
    table = key_ids + [blk, blk ^ 1, x, (x + side) % 4, (x - side) % 4, (x + 2) % 4, zl, c]
    ids = jnp.stack([jnp.asarray(v, jnp.int32) for v in table])

    mine = lax.dynamic_slice_in_dim(out_weight, c * 128, 128, 0)
    rest = lax.dynamic_slice_in_dim(out_weight, (1 - c) * 128, 128, 0)
    g1a = move(mine, x_out)
    g1b = move(rest, x_out)
    g2 = move(g1a, x_out)
    s1a, s1b, s2 = (move(g1a, core_swap), move(g1b, core_swap), move(g2, core_swap))
    state = flash(ids, 0, q_own, q_oth, kvs[:4], None, False)
    o_own, ml_own, o_oth, ml_oth = flash(ids, 4, q_own, q_oth, kvs[4:], state, True)
    o_in, ml_in = move(o_oth, core_swap), move(ml_oth, core_swap)
    t_0, t_out, t_in, t_2 = merge(ids, o_own, ml_own, o_in, ml_in)
    e_in = move(t_out, x_out)
    e_out = move(t_in, x_in)
    e_2 = move(t_2, x_by(2))
    atts, w_rest = [t_0, e_in, e_out, e_2], [g1a, g1b, s1b, s1a, g2, s2]
    own_s, oth_s = project(ids, atts, out_weight, w_rest, 0, 4096)
    got_s = move(oth_s, z_low_pair)
    residual, normed = residual_norm(hidden_in, own_s, got_s, norm_gain.reshape(1, 4096))

    n_a = move(normed, x_out)
    n_b = move(normed, x_in)
    z_0 = move(normed, z_pair)
    n_2 = move(n_a, x_out)
    z_a = move(n_a, z_pair)
    z_b = move(n_b, z_pair)
    z_2 = move(n_2, z_pair)
    weights = (gate_weight, up_weight, down_weight)
    near = mlp([normed, n_a, n_b, z_0], *weights)
    h_0 = [move(near[6 + i], z_pair) for i in range(2)]
    far = mlp([z_2, z_a, z_b, n_2], *weights)
    parts = []
    for i in range(2):
        p_0, p_a, p_b = near[i], near[2 + i], near[4 + i]
        f_2, f_a, f_b, p_2 = far[i], far[2 + i], far[4 + i], far[6 + i]
        h_2 = move(f_2, z_pair)
        h_a = move(f_a, z_pair)
        h_b = move(f_b, z_pair)
        r_2 = move(added(p_2, h_2), x_in)
        r_b = move(added(p_b, h_b), x_out)
        q_a = (p_a.astype(F32) + h_a.astype(F32) + r_2.astype(F32)).astype(BF)
        r_a = move(q_a, x_in)
        early = p_0.astype(F32) + h_0[i].astype(F32) + residual[:, i * 2048 : (i + 1) * 2048].astype(F32)
        parts.append(lax.optimization_barrier(early) + r_a.astype(F32) + r_b.astype(F32))
    return jnp.concatenate(parts, axis=1).astype(BF)


def solution(mesh):
    tok = P(("blk", "head"), None)
    return jax.shard_map(
        local,
        mesh=mesh,
        in_specs=(tok, tok, tok, tok, P("head", None), P(), P(None, "head"), P(None, "head"), P("head", None)),
        out_specs=tok,
        check_vma=False,
    )
```

```python
import functools

import jax
import jax.numpy as jnp
from jax import lax
from jax.experimental import pallas as pl
from jax.experimental.pallas import tpu as pltpu
from jax.sharding import PartitionSpec as P


HEAD_DIM = 128
BF = jnp.bfloat16
F32 = jnp.float32
NEG = -1e30
SCALE2 = HEAD_DIM**-0.5 * 1.4426950408889634
VLIM = 56 * 1024 * 1024
MLP_VLIM = 66_000_000


def flat(x, y, z, c):
    return ((z % 2) * 4 + x) * 16 + (z // 2) * 8 + y * 2 + c


def move(a, f):
    pairs = []
    for x in range(4):
        for y in range(4):
            for z in range(4):
                for c in range(2):
                    tx, ty, tz, tc = f(x, y, z, c)
                    pairs.append((flat(x, y, z, c), flat(tx % 4, ty % 4, tz % 4, tc)))
    return lax.ppermute(a, ("head", "blk"), pairs)


def x_by(d):
    return lambda x, y, z, c: (x + d, y, z, c)


def x_out(x, y, z, c):
    return (x + 1 if c == 0 else x - 1, y, z, c)


def x_in(x, y, z, c):
    return (x - 1 if c == 0 else x + 1, y, z, c)


def core_swap(x, y, z, c):
    return (x, y, z, 1 - c)


def z_low_pair(x, y, z, c):
    return (x, y, z ^ 1, c)


def z_pair(x, y, z, c):
    return (x, y, z ^ 1 if c == 0 else 3 - z, c)


def across(f):
    return lambda x, y, z, c: z_pair(*f(x, y, z, c))


def blk_by(dy, dz):
    return lambda x, y, z, c: (x, y + dy, z + 2 * dz, c)


ROWS = 128


GROUP = 2


def flash_body(q2, kk, va, m_ref, acc_ref, qi, heads, slots, reach):
    for h in heads:
        for r in range(512 // ROWS):
            rows = pl.ds(r * ROWS, ROWS)
            q = q2[qi, h, rows, :]
            ss = []
            for j in slots:
                s = lax.dot_general(q, kk[j], (((1,), (1,)), ((), ())), preferred_element_type=F32)
                if reach is not None:
                    ri = lax.broadcasted_iota(jnp.int32, s.shape, 0) + (r * ROWS + reach)
                    ci = lax.broadcasted_iota(jnp.int32, s.shape, 1)
                    s = jnp.where(ci <= ri, s, NEG)
                ss.append(s)
            top = ss[0]
            for s in ss[1:]:
                top = jnp.maximum(top, s)
            m_old = m_ref[qi, h, rows, :]
            m_new = jnp.maximum(m_old, jnp.max(top, axis=-1, keepdims=True) * SCALE2)
            pv = None
            for j, s in zip(slots, ss):
                p = jnp.exp2(s * SCALE2 - m_new[:, :1]).astype(BF)
                part = jnp.dot(p, va[j], preferred_element_type=F32)
                pv = part if pv is None else pv + part
            alpha = jnp.exp2(m_old - m_new)
            acc = acc_ref[qi, h, rows, :]
            acc_ref[qi, h, rows, :] = acc * jnp.concatenate([alpha, alpha], axis=1) + pv
            m_ref[qi, h, rows, :] = m_new


def flash_kernel(n, first, base, table, q_own, q_oth, *refs):
    ids = [table[base + j] for j in range(n)] + [table[8], table[9]]
    kvs, refs = refs[:n], refs[n:]
    if not first:
        init, refs = refs[:4], refs[4:]
    outs, (q2, kk, va, m_ref, acc_ref, vis) = refs[:4], refs[4:]
    for h in range(2):
        q2[0, h] = q_own[:, h * 128 : (h + 1) * 128]
        q2[1, h] = q_oth[:, h * 128 : (h + 1) * 128]
    for j in range(n):
        kk[j] = kvs[j][:, :128]
        va[j, :, :128] = kvs[j][:, 128:]
        va[j, :, 128:] = jnp.ones((512, 128), BF)
    if first:
        m_ref[...] = jnp.full(m_ref.shape, NEG, F32)
        acc_ref[...] = jnp.zeros(acc_ref.shape, F32)
    else:
        for qi in range(2):
            for h in range(2):
                lse = jnp.broadcast_to(init[2 * qi + 1][:, h : h + 1], (512, 128))
                m_ref[qi, h] = lse
                acc_ref[qi, h, :, :128] = init[2 * qi][:, h * 128 : (h + 1) * 128]
                acc_ref[qi, h, :, 128:] = jnp.where(lse > NEG, 1.0, 0.0)

    counts = []
    for qi in range(2):
        seen = jnp.int32(0)
        for j in range(n):
            vis[qi, seen] = j
            seen = seen + (ids[j] < ids[n + qi]).astype(jnp.int32)
        counts.append(seen)
    groups = [cnt // GROUP for cnt in counts]

    def grouped(t, carry):
        qi = (t >= groups[0]).astype(jnp.int32)
        at = (t - qi * groups[0]) * GROUP
        flash_body(q2, kk, va, m_ref, acc_ref, qi, (0, 1), [vis[qi, at + g] for g in range(GROUP)], None)
        return carry

    lax.fori_loop(0, groups[0] + groups[1], grouped, 0)
    rest = [cnt - g * GROUP for cnt, g in zip(counts, groups)]

    lead = 1 if first else 0

    def single(t, carry):
        u = t // 2 - lead
        qi = (u >= rest[0]).astype(jnp.int32)
        at = jnp.where(qi == 1, groups[1], groups[0]) * GROUP + u - qi * rest[0]
        own = u < 0
        slot = jnp.where(own, 0, vis[qi, jnp.maximum(at, 0)])
        reach = jnp.where(own, 0, 512)
        flash_body(q2, kk, va, m_ref, acc_ref, jnp.where(own, 0, qi), (t % 2,), [slot], reach)
        return carry

    lax.fori_loop(0, 2 * (rest[0] + rest[1] + lead), single, 0)
    lane = lax.broadcasted_iota(jnp.int32, (512, 128), 1)
    for qi in range(2):
        o_ref, ml = outs[2 * qi], outs[2 * qi + 1]
        lse = []
        for h in range(2):
            total = acc_ref[qi, h, :, 128:]
            seen = total > 0.0
            safe = jnp.where(seen, total, 1.0)
            o_ref[:, h * 128 : (h + 1) * 128] = (acc_ref[qi, h, :, :128] / safe).astype(o_ref.dtype)
            lse.append(jnp.where(seen, m_ref[qi, h] + jnp.log2(safe), NEG))
        ml[...] = jnp.where(lane == 0, lse[0], lse[1])


def flash(ids, base, q_own, q_oth, kvs, init=None, last=True):
    vm = pl.BlockSpec(memory_space=pltpu.VMEM)
    n = len(kvs)
    extra = [] if init is None else list(init)
    oth = BF if last else F32
    return pl.pallas_call(
        functools.partial(flash_kernel, n, init is None, base),
        in_specs=[pl.BlockSpec(memory_space=pltpu.SMEM)] + [vm] * (2 + n + len(extra)),
        out_specs=[vm] * 4,
        out_shape=[
            jax.ShapeDtypeStruct((512, 256), F32),
            jax.ShapeDtypeStruct((512, 128), F32),
            jax.ShapeDtypeStruct((512, 256), oth),
            jax.ShapeDtypeStruct((512, 128), F32),
        ],
        scratch_shapes=[
            pltpu.VMEM((2, 2, 512, 128), BF),
            pltpu.VMEM((n, 512, 128), BF),
            pltpu.VMEM((n, 512, 256), BF),
            pltpu.VMEM((2, 2, 512, 128), F32),
            pltpu.VMEM((2, 2, 512, 256), F32),
            pltpu.SMEM((2, n + 1), jnp.int32),
        ],
        compiler_params=pltpu.CompilerParams(vmem_limit_bytes=VLIM),
        cost_estimate=pl.CostEstimate(flops=1_100_000_000 * n, transcendentals=0, bytes_accessed=4 << 20),
    )(ids, q_own, q_oth, *kvs, *extra)


def merge_kernel(ids, o_own, ml_own, o_in, ml_in, *outs):
    for d, out in enumerate(outs):
        for zl in range(2):
            rows = pl.ds(pl.multiple_of(zl * 256 + ids[10 + d] * 64, 64), 64)
            for h in range(2):
                a = ml_own[rows, h : h + 1]
                b = ml_in[rows, h : h + 1]
                top = jnp.maximum(a, b)
                wa = jnp.exp2(a - top)
                wb = jnp.exp2(b - top)
                tot = wa + wb
                cols = slice(h * 128, (h + 1) * 128)
                res = o_own[rows, cols] * (wa / tot) + o_in[rows, cols].astype(F32) * (wb / tot)
                out[zl, :, cols] = res.astype(BF)


def merge(*args):
    vm = pl.BlockSpec(memory_space=pltpu.VMEM)
    return pl.pallas_call(
        merge_kernel,
        in_specs=[pl.BlockSpec(memory_space=pltpu.SMEM)] + [vm] * 4,
        out_specs=[vm] * 4,
        out_shape=[jax.ShapeDtypeStruct((2, 64, 256), BF)] * 4,
        cost_estimate=pl.CostEstimate(flops=1_000_000, transcendentals=0, bytes_accessed=1 << 20),
        name="merge",
    )(*args)


def proj_kernel(col, ids, att0, att1, att2, att3, own_w, *refs):
    atts, ws, (own, oth, wbuf, acc, sems) = (att0, att1, att2, att3), refs[:6], refs[6:]
    zl, c = ids[14], ids[15]
    width = own.shape[1]
    near, far = pl.multiple_of(c * 128, 128), pl.multiple_of((1 - c) * 128, 128)
    lo, hi = pl.ds(near, 128), pl.ds(far, 128)
    cut = pl.ds(col, width)
    copies = [(own_w.at[pl.ds(0, 256), cut], 0, pl.ds(0, 256))]
    copies += [(w.at[:, cut], p, d) for w, p, d in zip(ws, (1, 1, 2, 2, 3, 3), (lo, hi, lo, hi, lo, hi))]
    dmas = [pltpu.make_async_copy(src, wbuf.at[p, d], sems.at[i]) for i, (src, p, d) in enumerate(copies)]
    for d in dmas:
        d.start()
    for p in range(4):
        for i in (0,) if p == 0 else (2 * p - 1, 2 * p):
            dmas[i].wait()
        att = atts[p]
        a = jnp.concatenate([att[zl], att[1 - zl]], axis=0)
        part = jnp.dot(a, wbuf[p], preferred_element_type=F32)
        if p == 0:
            acc[...] = part
        else:
            acc[...] += part
    own[...] = acc[:64]
    oth[...] = acc[64:].astype(BF)


def project(ids, atts, own_w, ws, col, width):
    vm = pl.BlockSpec(memory_space=pltpu.VMEM)
    hb = pl.BlockSpec(memory_space=pltpu.HBM)
    return pl.pallas_call(
        functools.partial(proj_kernel, col),
        in_specs=[pl.BlockSpec(memory_space=pltpu.SMEM)] + [vm] * 4 + [hb] * 7,
        out_specs=[vm] * 2,
        out_shape=[jax.ShapeDtypeStruct((64, width), F32), jax.ShapeDtypeStruct((64, width), BF)],
        scratch_shapes=[
            pltpu.VMEM((4, 256, width), BF),
            pltpu.VMEM((128, width), F32),
            pltpu.SemaphoreType.DMA((7,)),
        ],
        compiler_params=pltpu.CompilerParams(vmem_limit_bytes=VLIM),
        cost_estimate=pl.CostEstimate(flops=550_000_000, transcendentals=0, bytes_accessed=4 << 20),
    )(ids, *atts, own_w, *ws)


def norm_kernel(hid, own, got, gain, res_out, nrm_out):
    res = (hid[...].astype(F32) + (own[...] + got[...].astype(F32))).astype(BF)
    res_out[...] = res
    wide = res.astype(F32)
    ms = jnp.mean(wide * wide, axis=-1, keepdims=True)
    nrm_out[...] = (wide * lax.rsqrt(ms + 1e-05) * gain[...]).astype(BF)


def residual_norm(*args):
    vm = pl.BlockSpec(memory_space=pltpu.VMEM)
    return pl.pallas_call(
        norm_kernel,
        in_specs=[vm] * 4,
        out_specs=[vm] * 2,
        out_shape=[jax.ShapeDtypeStruct((64, 4096), BF)] * 2,
        cost_estimate=pl.CostEstimate(flops=2_000_000, transcendentals=0, bytes_accessed=3 << 20),
        name="norm",
    )(*args)


KC = 1024
DEPTH = 4


def mlp_kernel(n_in, *refs):
    xs, (wg, wu, wd), outs = refs[:n_in], refs[n_in : n_in + 3], refs[n_in + 3 : 3 * n_in + 3]
    wbuf, dbuf, acc, xbuf, obuf, sems, xsems, osems = refs[3 * n_in + 3 :]
    nk = 4096 // KC
    order = []
    for k in range(nk):
        rows = pl.ds(k * KC, KC)
        order.append(pltpu.make_async_copy(wg.at[rows], wbuf.at[k, :, pl.ds(0, 896)], sems.at[2 * k]))
        order.append(pltpu.make_async_copy(wu.at[rows], wbuf.at[k, :, pl.ds(896, 896)], sems.at[2 * k + 1]))
    order += [
        pltpu.make_async_copy(wd.at[:, pl.ds(n * 1024, 1024)], dbuf.at[n], sems.at[2 * nk + n]) for n in range(4)
    ]
    loads = [pltpu.make_async_copy(r, xbuf.at[pl.ds(i * 64, 64)], xsems.at[i]) for i, r in enumerate(xs)]
    for d in loads + order[:DEPTH]:
        d.start()

    def settle(at, count):
        for i in range(at, at + count):
            order[i].wait()
        for i in range(at + DEPTH, min(at + DEPTH + count, len(order))):
            order[i].start()

    for d in loads:
        d.wait()
    for k in range(nk):
        settle(2 * k, 2)
        part = jnp.dot(xbuf[:, k * KC : (k + 1) * KC], wbuf[k], preferred_element_type=F32)
        if k == 0:
            acc[...] = part
        else:
            acc[...] += part
    gate = acc[:, :896]
    inner = (gate / (1.0 + jnp.exp(-gate)) * acc[:, 896:]).astype(BF)
    stores = []
    for n in range(4):
        settle(2 * nk + n, 1)
        cols = pl.ds(n * 1024, 1024)
        obuf[:, n * 1024 : (n + 1) * 1024] = jnp.dot(inner, dbuf[n], preferred_element_type=F32).astype(BF)
        at = pl.ds(n % 2 * 1024, 1024)
        for i in range(n_in):
            o = outs[2 * i + n // 2]
            d = pltpu.make_async_copy(obuf.at[pl.ds(i * 64, 64), cols], o.at[:, at], osems.at[n, i])
            d.start()
            stores.append(d)
    for d in stores:
        d.wait()


def mlp(xs, wg, wu, wd):
    hb = pl.BlockSpec(memory_space=pltpu.HBM)
    n_in = len(xs)
    return pl.pallas_call(
        functools.partial(mlp_kernel, n_in),
        in_specs=[hb] * (n_in + 3),
        out_specs=[hb] * (2 * n_in),
        out_shape=[jax.ShapeDtypeStruct((64, 2048), BF)] * (2 * n_in),
        scratch_shapes=[
            pltpu.VMEM((4096 // KC, KC, 1792), BF),
            pltpu.VMEM((4, 896, 1024), BF),
            pltpu.VMEM((n_in * 64, 1792), F32),
            pltpu.VMEM((n_in * 64, 4096), BF),
            pltpu.VMEM((n_in * 64, 4096), BF),
            pltpu.SemaphoreType.DMA((2 * (4096 // KC) + 4,)),
            pltpu.SemaphoreType.DMA((n_in,)),
            pltpu.SemaphoreType.DMA((4, n_in)),
        ],
        compiler_params=pltpu.CompilerParams(vmem_limit_bytes=MLP_VLIM),
        cost_estimate=pl.CostEstimate(flops=5_640_000_000, transcendentals=0, bytes_accessed=26 << 20),
    )(*xs, wg, wu, wd)


def added(a, b):
    return (a.astype(F32) + b.astype(F32)).astype(BF)


def pack_kernel(q, k, v, out):
    for h in range(8):
        out[h, :, :256] = q[:, h * 256 : (h + 1) * 256]
        out[h, :, 256:384] = k[:, h * 128 : (h + 1) * 128]
        out[h, :, 384:] = v[:, h * 128 : (h + 1) * 128]


def exchange_qkv(queries, key_states, value_states):
    vm = pl.BlockSpec(memory_space=pltpu.VMEM)
    both = pl.pallas_call(
        pack_kernel,
        in_specs=[vm] * 3,
        out_specs=vm,
        out_shape=jax.ShapeDtypeStruct((8, 64, 512), BF),
        cost_estimate=pl.CostEstimate(flops=1_000_000, transcendentals=0, bytes_accessed=1 << 20),
        name="pack",
    )(queries, key_states, value_states)
    got = lax.all_to_all(both, "head", split_axis=0, concat_axis=0, tiled=True)
    got = got.reshape(512, 512)
    return got[:, :256], got[:, 256:]


def local(hidden_in, queries, key_states, value_states, out_weight, norm_gain, gate_weight, up_weight, down_weight):
    head = lax.axis_index("head")
    blk = lax.axis_index("blk")
    x, zl = head % 4, head // 4
    c, y, zh = blk % 2, (blk // 2) % 4, blk // 8

    q_own, kv = exchange_qkv(queries, key_states, value_states)

    steps = [(1, 0), (-1, 0), (0, 1), (2, 0), (1, 1), (-1, 1), (2, 1)]
    kvs, key_ids = [kv], [blk]
    for dy, dz in steps:
        kvs.append(move(kv, blk_by(dy, dz)))
        key_ids.append((zh ^ dz) * 8 + ((y - dy) % 4) * 2 + c)
    q_oth = move(q_own, core_swap)
    side = jnp.where(c == 0, 1, -1)
    table = key_ids + [blk, blk ^ 1, x, (x + side) % 4, (x - side) % 4, (x + 2) % 4, zl, c]
    ids = jnp.stack([jnp.asarray(v, jnp.int32) for v in table])

    mine = lax.dynamic_slice_in_dim(out_weight, c * 128, 128, 0)
    rest = lax.dynamic_slice_in_dim(out_weight, (1 - c) * 128, 128, 0)
    g1a = move(mine, x_out)
    g1b = move(rest, x_out)
    g2 = move(g1a, x_out)
    s1a, s1b, s2 = (move(g1a, core_swap), move(g1b, core_swap), move(g2, core_swap))
    state = flash(ids, 0, q_own, q_oth, kvs[:4], None, False)
    o_own, ml_own, o_oth, ml_oth = flash(ids, 4, q_own, q_oth, kvs[4:], state, True)
    o_in, ml_in = move(o_oth, core_swap), move(ml_oth, core_swap)
    t_0, t_out, t_in, t_2 = merge(ids, o_own, ml_own, o_in, ml_in)
    e_in = move(t_out, x_out)
    e_out = move(t_in, x_in)
    e_2 = move(t_2, x_by(2))
    atts, w_rest = [t_0, e_in, e_out, e_2], [g1a, g1b, s1b, s1a, g2, s2]
    own_s, oth_s = project(ids, atts, out_weight, w_rest, 0, 4096)
    got_s = move(oth_s, z_low_pair)
    residual, normed = residual_norm(hidden_in, own_s, got_s, norm_gain.reshape(1, 4096))

    n_a = move(normed, x_out)
    n_b = move(normed, x_in)
    z_0 = move(normed, z_pair)
    n_2 = move(n_a, x_out)
    z_a = move(n_a, z_pair)
    z_b = move(n_b, z_pair)
    z_2 = move(normed, across(x_by(2)))
    weights = (gate_weight, up_weight, down_weight)
    near = mlp([normed, n_a, n_b, z_0], *weights)
    h_0 = [move(near[6 + i], z_pair) for i in range(2)]
    far = mlp([z_2, z_a, z_b, n_2], *weights)
    parts = []
    for i in range(2):
        p_0, p_a, p_b = near[i], near[2 + i], near[4 + i]
        f_2, f_a, f_b, p_2 = far[i], far[2 + i], far[4 + i], far[6 + i]
        h_2 = move(f_2, z_pair)
        h_a = move(f_a, z_pair)
        h_b = move(f_b, z_pair)
        r_2 = move(added(p_2, h_2), x_in)
        r_b = move(added(p_b, h_b), x_out)
        q_a = (p_a.astype(F32) + h_a.astype(F32) + r_2.astype(F32)).astype(BF)
        r_a = move(q_a, x_in)
        early = p_0.astype(F32) + h_0[i].astype(F32) + residual[:, i * 2048 : (i + 1) * 2048].astype(F32)
        parts.append(lax.optimization_barrier(early) + r_a.astype(F32) + r_b.astype(F32))
    return jnp.concatenate(parts, axis=1).astype(BF)


def solution(mesh):
    tok = P(("blk", "head"), None)
    return jax.shard_map(
        local,
        mesh=mesh,
        in_specs=(tok, tok, tok, tok, P("head", None), P(), P(None, "head"), P(None, "head"), P("head", None)),
        out_specs=tok,
        check_vma=False,
    )
```
